32 devices in a mesh: pc: 8 (over z, y), pr: 4 (over x, core).
Axes of the slice: x: 2, y: 2, z: 4, core: 2. Of those that a mesh axis runs over, the one named last changes fastest.
Arguments:
- panel_in: float32 [4096, 24, 128], P('pr', 'pc')
- trail_in: float32 [4096, 1024], P('pr', 'pc')
Outputs:
- output 1: float32 [4096, 24, 128], P('pr', 'pc')
- output 2: float32 [4096, 1024], P('pr', 'pc')
All inputs are finite; a program needn't handle non-finite values.
Results may differ from the reference program's by a relative error of at most 0.001.
Values sent between devices are 32-bit elements.
A program may use at most 1 GiB of HBM per device.

```python
import jax
import jax.numpy as jnp
from jax import lax

N = 4096
NB = 128
K = 24
PR = 4
PC = 8
RANK = 2048

BLOCKS = N // NB
ROW_BLOCKS = BLOCKS // PR
TRAIL_COLS = N - K * NB
PREC_HIGH = lax.Precision.HIGHEST


def rows_to_owner(full_mat):
    col_width = full_mat.shape[1]
    return full_mat.reshape(ROW_BLOCKS, PR, NB, col_width).transpose(1, 0, 2, 3).reshape(N, col_width)


def rows_from_owner(stored):
    col_width = stored.shape[1]
    return stored.reshape(PR, ROW_BLOCKS, NB, col_width).transpose(1, 0, 2, 3).reshape(N, col_width)


def cols_to_owner(full_mat):
    block_count = full_mat.shape[1] // NB
    return full_mat.reshape(N, block_count // PC, PC, NB).transpose(0, 2, 1, 3).reshape(N, block_count, NB)


def cols_from_owner(stored):
    block_count = stored.shape[1]
    return stored.reshape(N, PC, block_count // PC, NB).transpose(0, 2, 1, 3).reshape(N, block_count * NB)


def build_layout(full_mat):
    row_major = rows_to_owner(full_mat)
    panel_in = cols_to_owner(row_major[:, :K * NB])
    trail_in = cols_to_owner(row_major[:, K * NB:]).reshape(N, TRAIL_COLS)
    return {"panel_in": panel_in, "trail_in": trail_in}


def setup_inputs(seed: int = 0) -> dict:
    key_low, key_diag = jax.random.split(jax.random.key(seed))
    factor = jax.random.normal(key_low, (N, RANK), jnp.float32)
    diag_shift = 0.5 + jax.random.uniform(key_diag, (N,), jnp.float32)
    low_rank = jnp.dot(factor, factor.T, precision=PREC_HIGH) / RANK
    full_mat = 0.5 * (low_rank + low_rank.T) + jnp.diag(diag_shift)
    return build_layout(full_mat)


def reference(panel_in, trail_in):
    stored = jnp.concatenate([cols_from_owner(panel_in), cols_from_owner(trail_in.reshape(N, BLOCKS - K, NB))], axis=1)
    work_mat = rows_from_owner(stored)
    factor_cols = []
    kept_rows = []
    for panel_step in range(K):
        l_diag = jnp.linalg.cholesky(work_mat[:NB, :NB])
        below_diag = lax.linalg.triangular_solve(l_diag, work_mat[NB:, :NB], left_side=False, lower=True, transpose_a=True)
        factor_cols.append(jnp.concatenate([jnp.zeros((panel_step * NB, NB), work_mat.dtype), l_diag, below_diag], axis=0))
        kept_rows.append(work_mat[:NB, (K - panel_step) * NB:])
        work_mat = work_mat[NB:, NB:] - jnp.dot(below_diag, below_diag.T, precision=PREC_HIGH)
    panel_full = jnp.concatenate(factor_cols, axis=1)
    trail_full = jnp.concatenate(kept_rows + [work_mat], axis=0)
    panel_out = cols_to_owner(rows_to_owner(panel_full))
    trail_out = cols_to_owner(rows_to_owner(trail_full)).reshape(N, TRAIL_COLS)
    return panel_out, trail_out
```

```python
import jax
import jax.numpy as jnp
from jax import lax
from jax.experimental import pallas as pl
from jax.experimental.pallas import tpu as pltpu
from jax.sharding import PartitionSpec as P

MESH = pl.DeviceIdType.MESH
PREC_HIGH = lax.Precision.HIGHEST
NB = 128
LAG = 3
CHAIN_COL = 2
CHAIN_ROW = 1
RING = 8


def _sub_bcast(v, s):
    return jnp.broadcast_to(v[s:s + 1, :], (8, NB))


def _lane_bcast(v, c):
    return jnp.broadcast_to(v[:, c:c + 1], (8, NB))


def chol_inv(load, store_l, store_inv, q=2):
    ng = NB // 8
    step = 8 * q
    x = [load(g) for g in range(ng)]
    row_id = lax.broadcasted_iota(jnp.int32, (8, NB), 0)
    col_id = lax.broadcasted_iota(jnp.int32, (8, NB), 1)
    y = [jnp.where(col_id == row_id + 8 * g, 1.0, 0.0) for g in range(ng)]
    for b in range(NB // step):
        g0 = b * q
        c0 = b * step
        last = b == NB // step - 1
        e = [[_lane_bcast(x[g0 + s], c0 + t) if 8 * (s + 1) > t else None for s in range(q)] for t in range(step)]
        p = None
        if not last:
            p = [[_lane_bcast(x[g0 + q + s], c0 + t) for s in range(q)] for t in range(step)]
        rr = [None] * q
        ss = [None] * q
        rows = []
        for t in range(step):
            gt, st = t // 8, t % 8
            d = _sub_bcast(e[t][gt], st)
            r = lax.rsqrt(d)
            col = [e[t][s] * r if s >= gt else None for s in range(q)]
            rt = _sub_bcast(x[g0 + gt], st) * r
            sr = _sub_bcast(y[g0 + gt], st) * r
            rows.append((rt, sr))
            if st == 0:
                rr[gt], ss[gt] = rt, sr
            else:
                rr[gt] = jnp.where(row_id == st, rt, rr[gt])
                ss[gt] = jnp.where(row_id == st, sr, ss[gt])
            for s in range(gt, q):
                x[g0 + s] = x[g0 + s] - col[s] * rt
                y[g0 + s] = y[g0 + s] - col[s] * sr
            pc = None
            if not last:
                pc = [p[t][s] * r for s in range(q)]
                for s in range(q):
                    x[g0 + q + s] = x[g0 + q + s] - pc[s] * rt
                    y[g0 + q + s] = y[g0 + q + s] - pc[s] * sr
            for u in range(t + 1, step):
                w = _sub_bcast(col[u // 8], u % 8)
                for s in range(u // 8, q):
                    e[u][s] = e[u][s] - col[s] * w
                if not last:
                    for s in range(q):
                        p[u][s] = p[u][s] - pc[s] * w
        for s in range(q):
            store_l(g0 + s, jnp.where(col_id >= row_id + 8 * (g0 + s), rr[s], 0.0))
            store_inv(g0 + s, jnp.where(col_id <= row_id + 8 * (g0 + s), ss[s], 0.0))
        if b < NB // step - 2:
            for s in range(q):
                rt_t = jnp.transpose(rr[s])
                for g in range(g0 + 2 * q, ng):
                    blk = rt_t[8 * g:8 * g + 8, :]
                    for st in range(8):
                        m = jnp.broadcast_to(blk[:, st:st + 1], (8, NB))
                        rt, sr = rows[8 * s + st]
                        x[g] = x[g] - m * rt
                        y[g] = y[g] - m * sr


def dot_nt(a, b):
    return lax.dot_general(a, b, (((1,), (1,)), ((), ())), precision=PREC_HIGH, preferred_element_type=jnp.float32)


def make_kernel(row_procs, col_procs, local_rows, panel_dev):
    steps = panel_dev * col_procs
    row_blocks = local_rows // NB
    slots = panel_dev + 1
    half = row_blocks // 2
    sib_row = CHAIN_ROW ^ 1

    def kernel(pan_in, trl_in, pan_out, trl_out, tile, rowp, colp, linv_in, ldiag_in, stage, win, lwin, linv_c, lt_c, diag,
               in_sem, row_sem, col_sem, linv_sem, ldiag_sem, win_sem, outc_sem, out_sem,
               row_snd, col_snd, stage_snd, init_snd, linv_snd, ldiag_snd, give_snd, give_sem):
        pc = lax.axis_index("pc")
        pr = lax.axis_index("pr")
        at_chain_col = pc == CHAIN_COL
        is_chain = jnp.logical_and(at_chain_col, pr == CHAIN_ROW)
        is_sib = jnp.logical_and(at_chain_col, pr == sib_row)
        chain_id = (CHAIN_COL, CHAIN_ROW)
        sib_id = (CHAIN_COL, sib_row)
        some_other = (pc, pr ^ 1)

        def rows(l):
            return pl.ds(pl.multiple_of(l * NB, NB), NB)

        def remote(src, dst, snd, rcv, dev):
            return pltpu.make_async_remote_copy(src_ref=src, dst_ref=dst, send_sem=snd, recv_sem=rcv, device_id=dev, device_id_type=MESH)

        def wait_recv(ref, rcv):
            remote(ref, ref, give_snd.at[0], rcv, some_other).wait_recv()

        barrier = pltpu.get_barrier_semaphore()
        total = row_procs * col_procs
        me = pc * row_procs + pr

        def greet(d, _):
            other = lax.rem(me + d, total)
            pl.semaphore_signal(barrier, inc=1, device_id=(other // row_procs, lax.rem(other, row_procs)), device_id_type=MESH)
            return 0

        def load(m):
            src = pan_in.at[m] if m < panel_dev else trl_in
            return pltpu.make_async_copy(src, tile.at[0, m], in_sem.at[m])

        @pl.when(jnp.logical_not(is_chain))
        def _():
            for m in range(slots):
                load(m).start()

        lax.fori_loop(1, total, greet, 0)
        pl.semaphore_wait(barrier, total - 1)

        def give(m):
            src = pan_in.at[m] if m < panel_dev else trl_in
            return remote(src, tile.at[1, m], give_snd.at[m], give_sem.at[m], sib_id)

        def linv_copy(i, r):
            return remote(linv_c.at[lax.rem(i, RING)], linv_in.at[i // col_procs], linv_snd.at[lax.rem(i, 2), r], linv_sem.at[i // col_procs],
                          (lax.rem(i, col_procs), r))

        def linv_goes(i, r):
            return jnp.logical_or(lax.rem(i, col_procs) != CHAIN_COL, r != CHAIN_ROW)

        def ldiag_copy(i):
            return remote(lt_c.at[i], ldiag_in.at[i // col_procs], ldiag_snd.at[lax.rem(i, 2)], ldiag_sem.at[i // col_procs],
                          (lax.rem(i, col_procs), lax.rem(i, row_procs)))

        def drain_chain(i):
            for r in range(row_procs):
                @pl.when(linv_goes(i, r))
                def _():
                    linv_copy(i, r).wait_send()
            ldiag_copy(i).wait_send()

        def chain_step(i, _):
            for s in range(LAG + 1):
                @pl.when(i - LAG + s >= 0)
                def _():
                    wait_recv(win.at[i, s], win_sem.at[i, s])
            at = lax.rem(i, RING)
            old = [lax.rem(i + RING - LAG + s, RING) for s in range(LAG)]
            for s in range(LAG):
                acc = win[i, s]
                for q in range(s):
                    acc = acc - dot_nt(lwin[at, q], lwin[old[s], LAG - s + q])
                lwin[at, s] = dot_nt(acc, linv_c[old[s]])
            new_diag = win[i, LAG]
            for s in range(LAG):
                new_diag = new_diag - dot_nt(lwin[at, s], lwin[at, s])
            diag[...] = new_diag

            def put_l(g, v):
                lt_c[i, 8 * g:8 * g + 8, :] = v

            def put_inv(g, v):
                linv_c[at, 8 * g:8 * g + 8, :] = v

            chol_inv(lambda g: diag[8 * g:8 * g + 8, :], put_l, put_inv)

            @pl.when(i >= 2)
            def _():
                drain_chain(i - 2)

            for r in range(row_procs):
                @pl.when(linv_goes(i, r))
                def _():
                    linv_copy(i, r).start()
            ldiag_copy(i).start()
            return 0

        @pl.when(is_chain)
        def _():
            for m in range(slots):
                give(m).start()
            for i in range(RING):
                linv_c[i] = jnp.zeros((NB, NB), jnp.float32)
                for s in range(LAG):
                    lwin[i, s] = jnp.zeros((NB, NB), jnp.float32)
            for i in range(LAG):
                for s in range(LAG - i):
                    win[i, s] = jnp.zeros((NB, NB), jnp.float32)
            lax.fori_loop(0, steps, chain_step, 0)
            drain_chain(steps - 2)
            drain_chain(steps - 1)
            for m in range(slots):
                give(m).wait_send()
            for m in range(slots):
                dst = pan_out.at[m] if m < panel_dev else trl_out
                wait_recv(dst, outc_sem.at[m])

        num_virtual = jnp.where(is_sib, 2, 1)
        col_half = pc // row_procs
        z_me, y_me = pc // 2, lax.rem(pc, 2)
        is_col_src = pr == lax.rem(pc, row_procs)

        def row_of(v):
            return jnp.where(v == 0, pr, CHAIN_ROW)

        def first_block(k, r):
            return (k - r + row_procs) // row_procs

        def row_children(k):
            owner = lax.rem(k, col_procs)
            z_own, y_own = owner // 2, lax.rem(owner, 2)
            to_y = pc == owner
            to_up = jnp.logical_and(z_me >= z_own, z_me < col_procs // 2 - 1)
            to_down = jnp.logical_and(z_me <= z_own, z_me > 0)
            return ((to_y, z_me * 2 + 1 - y_me), (to_up, pc + 2), (to_down, pc - 2))

        def row_copy(k, v, l, c, peer):
            r = row_of(v)
            moved = jnp.logical_and(peer == CHAIN_COL, r == CHAIN_ROW)
            v_dst = jnp.where(moved, 1, 0)
            r_dst = jnp.where(moved, sib_row, r)
            return remote(rowp.at[v, k, rows(l)], rowp.at[v_dst, k, rows(l)], row_snd.at[lax.rem(k, 2), v, l, c],
                          row_sem.at[v_dst, k, l], (peer, r_dst))

        def col_copy(k, v, l, m, d):
            return remote(rowp.at[v, k, rows(l)], colp.at[k, rows(m)], col_snd.at[lax.rem(k, 2), m, d - 1],
                          col_sem.at[k, m], (pc, lax.rem(pr + d, row_procs)))

        def col_goes(d):
            return jnp.logical_not(jnp.logical_and(at_chain_col, lax.rem(pr + d, row_procs) == CHAIN_ROW))

        def is_col_block(v, l):
            return jnp.logical_and(row_of(v) == lax.rem(pc, row_procs), lax.rem(l, 2) == col_half)

        def each_block(k, act):
            def virtual(v, _):
                def block(l, _):
                    act(v, l)
                    return 0
                return lax.fori_loop(first_block(k, row_of(v)), row_blocks, block, 0)
            lax.fori_loop(0, num_virtual, virtual, 0)

        def each_send(k, v, l, act):
            for c, (goes, peer) in enumerate(row_children(k)):
                @pl.when(goes)
                def _():
                    act(row_copy(k, v, l, c, peer))

            @pl.when(is_col_block(v, l))
            def _():
                for d in range(1, row_procs):
                    @pl.when(col_goes(d))
                    def _():
                        act(col_copy(k, v, l, l // 2, d))

        def drain_sends(k):
            each_block(k, lambda v, l: each_send(k, v, l, lambda c: c.wait_send()))

        def stage_copy(v, i, s):
            return remote(stage.at[v, i // row_procs], win.at[i, s], stage_snd.at[v, i // row_procs], win_sem.at[i, s], chain_id)

        def entering(k, v):
            i = k + LAG + 1
            s = lax.rem(pc - (k + 1) + 4 * col_procs, col_procs)
            here = jnp.logical_and(jnp.logical_and(i < steps, s <= LAG), row_of(v) == lax.rem(i, row_procs))
            return here, i, s, (k + 1 + s) // col_procs

        def init_copy(i):
            return remote(pan_in.at[0, pl.ds((i // row_procs) * NB, NB)], win.at[i, jnp.clip(pc - i + LAG, 0, LAG)], init_snd.at[i],
                          win_sem.at[i, jnp.clip(pc - i + LAG, 0, LAG)], chain_id)

        def init_goes(i):
            return jnp.logical_and(pr == i % row_procs, pc <= i)

        def out_local(m):
            dst = pan_out.at[m] if m < panel_dev else trl_out
            return pltpu.make_async_copy(tile.at[0, m], dst, out_sem.at[m])

        def out_remote(m):
            dst = pan_out.at[m] if m < panel_dev else trl_out
            return remote(tile.at[1, m], dst, out_sem.at[slots + m], outc_sem.at[m], chain_id)

        def start_out(m):
            out_local(m).start()

            @pl.when(is_sib)
            def _():
                out_remote(m).start()

        def owner_step(k, _):
            own = pc == lax.rem(k, col_procs)
            m_own = k // col_procs

            @pl.when(k >= 2)
            def _():
                drain_sends(k - 2)

            @pl.when(own)
            def _():
                wait_recv(linv_in.at[m_own], linv_sem.at[m_own])

            def panel(v, l):
                @pl.when(own)
                def _():
                    x = dot_nt(tile[v, m_own, rows(l), :], linv_in[m_own])
                    rowp[v, k, rows(l), :] = x
                    tile[v, m_own, rows(l), :] = x

                @pl.when(jnp.logical_not(own))
                def _():
                    wait_recv(rowp.at[v, k, rows(l)], row_sem.at[v, k, l])

                each_send(k, v, l, lambda c: c.start())

                @pl.when(is_col_block(v, l))
                def _():
                    colp[k, rows(l // 2), :] = rowp[v, k, rows(l), :]

            each_block(k, panel)

            has_src = jnp.logical_or(is_col_src, jnp.logical_and(is_sib, CHAIN_ROW == lax.rem(pc, row_procs)))
            for m in range(slots):
                @pl.when(jnp.logical_and(jnp.logical_not(has_src), pc + m * col_procs > k))
                def _():
                    wait_recv(colp.at[k, m * NB:(m + 1) * NB], col_sem.at[k, m])

            def enter(v, _):
                here, i, s, m = entering(k, v)

                @pl.when(here)
                def _():
                    l = i // row_procs
                    new = tile[v, m, rows(l), :] - dot_nt(rowp[v, k, rows(l), :], colp[k, rows(m), :])
                    tile[v, m, rows(l), :] = new
                    stage[v, l] = new
                    stage_copy(v, i, s).start()
                return 0

            lax.fori_loop(0, num_virtual, enter, 0)

            def update(v, _):
                r = row_of(v)
                here, i, s, m_in = entering(k, v)
                l_in = jnp.where(here, i // row_procs, -1)
                first = first_block(k, r)
                for m in range(slots):
                    col_block = pc + m * col_procs
                    low = first
                    if m < panel_dev:
                        low = jnp.maximum(first, (col_block - r + row_procs - 1) // row_procs)
                    for h in range(2):
                        @pl.when(jnp.logical_and(col_block > k, low < (h + 1) * half))
                        def _():
                            part = pl.ds(h * half * NB, half * NB)
                            upd = dot_nt(rowp[v, k, part, :], colp[k, m * NB:(m + 1) * NB, :])
                            for b in range(half):
                                l = h * half + b
                                take = jnp.logical_and(l >= low, jnp.logical_or(m_in != m, l_in != l))
                                blk = slice(l * NB, (l + 1) * NB)
                                tile[v, m, blk, :] = tile[v, m, blk, :] - jnp.where(take, upd[b * NB:(b + 1) * NB], 0.0)
                return 0

            lax.fori_loop(0, num_virtual, update, 0)

            @pl.when(own)
            def _():
                def finish(v, _):
                    r = row_of(v)

                    @pl.when(r == lax.rem(k, row_procs))
                    def _():
                        wait_recv(ldiag_in.at[m_own], ldiag_sem.at[m_own])
                        tile[v, m_own, rows(k // row_procs), :] = jnp.transpose(ldiag_in[m_own])

                    def clear(l, _):
                        tile[v, m_own, rows(l), :] = jnp.zeros((NB, NB), jnp.float32)
                        return 0

                    lax.fori_loop(0, (k - r + row_procs - 1) // row_procs, clear, 0)
                    return 0

                lax.fori_loop(0, num_virtual, finish, 0)
                for m in range(panel_dev):
                    @pl.when(m_own == m)
                    def _():
                        start_out(m)
            return 0

        @pl.when(jnp.logical_not(is_chain))
        def _():
            for i in range(LAG + 1):
                @pl.when(init_goes(i))
                def _():
                    init_copy(i).start()
            for m in range(slots):
                load(m).wait()

            @pl.when(is_sib)
            def _():
                for m in range(slots):
                    wait_recv(tile.at[1, m], give_sem.at[m])

            lax.fori_loop(0, steps, owner_step, 0)
            start_out(panel_dev)
            drain_sends(steps - 2)
            drain_sends(steps - 1)
            for i in range(LAG + 1):
                @pl.when(init_goes(i))
                def _():
                    init_copy(i).wait_send()

            def drain_stage(k, _):
                def virtual(v, _):
                    here, i, s, m = entering(k, v)

                    @pl.when(here)
                    def _():
                        stage_copy(v, i, s).wait_send()
                    return 0
                return lax.fori_loop(0, num_virtual, virtual, 0)

            lax.fori_loop(0, steps, drain_stage, 0)
            for m in range(slots):
                out_local(m).wait()

                @pl.when(is_sib)
                def _():
                    out_remote(m).wait_send()

    return kernel


def solution(mesh):
    row_procs = mesh.shape["pr"]
    col_procs = mesh.shape["pc"]

    def local_part(panel_tile, trail_tile):
        local_rows, panel_dev, _ = panel_tile.shape
        steps = panel_dev * col_procs
        row_blocks = local_rows // NB
        slots = panel_dev + 1
        f32 = jnp.float32
        dma = pltpu.SemaphoreType.DMA
        scratch = [
            pltpu.VMEM((2, slots, local_rows, NB), f32),
            pltpu.VMEM((2, steps, local_rows, NB), f32),
            pltpu.VMEM((steps, slots * NB, NB), f32),
            pltpu.VMEM((panel_dev, NB, NB), f32),
            pltpu.VMEM((panel_dev, NB, NB), f32),
            pltpu.VMEM((2, steps // row_procs, NB, NB), f32),
            pltpu.VMEM((steps, LAG + 1, NB, NB), f32),
            pltpu.VMEM((RING, LAG, NB, NB), f32),
            pltpu.VMEM((RING, NB, NB), f32),
            pltpu.VMEM((steps, NB, NB), f32),
            pltpu.VMEM((NB, NB), f32),
            dma((slots,)),
            dma((2, steps, row_blocks)),
            dma((steps, slots)),
            dma((panel_dev,)),
            dma((panel_dev,)),
            dma((steps, LAG + 1)),
            dma((slots,)),
            dma((2 * slots,)),
            dma((2, 2, row_blocks, 3)),
            dma((2, slots, row_procs - 1)),
            dma((2, steps // row_procs)),
            dma((LAG + 1,)),
            dma((2, row_procs)),
            dma((2,)),
            dma((slots,)),
            dma((slots,)),
        ]
        hbm = pl.BlockSpec(memory_space=pl.ANY)
        by_slot = jnp.transpose(panel_tile, (1, 0, 2))
        panel_new, trail_new = pl.pallas_call(
            make_kernel(row_procs, col_procs, local_rows, panel_dev),
            out_shape=[jax.ShapeDtypeStruct(by_slot.shape, f32), jax.ShapeDtypeStruct(trail_tile.shape, f32)],
            in_specs=[hbm, hbm],
            out_specs=[hbm, hbm],
            scratch_shapes=scratch,
            compiler_params=pltpu.CompilerParams(collective_id=0, has_side_effects=True, vmem_limit_bytes=67043328),
        )(by_slot, trail_tile)
        return jnp.transpose(panel_new, (1, 0, 2)), trail_new

    spec_panel = P("pr", "pc", None)
    spec_trail = P("pr", "pc")
    return jax.shard_map(local_part, mesh=mesh, in_specs=(spec_panel, spec_trail), out_specs=(spec_panel, spec_trail), check_vma=False)
```

```python
import jax
import jax.numpy as jnp
from jax import lax
from jax.experimental import pallas as pl
from jax.experimental.pallas import tpu as pltpu
from jax.sharding import PartitionSpec as P

MESH = pl.DeviceIdType.MESH
PREC_HIGH = lax.Precision.HIGHEST
NB = 128
LAG = 3
CHAIN_COL = 2
CHAIN_ROW = 1
RING = 8


def _sub_bcast(v, s):
    return jnp.broadcast_to(v[s:s + 1, :], (8, NB))


def _lane_bcast(v, c):
    return jnp.broadcast_to(v[:, c:c + 1], (8, NB))


def chol_inv(load, store_l, store_inv, q=2):
    ng = NB // 8
    step = 8 * q
    x = [load(g) for g in range(ng)]
    row_id = lax.broadcasted_iota(jnp.int32, (8, NB), 0)
    col_id = lax.broadcasted_iota(jnp.int32, (8, NB), 1)
    y = [jnp.where(col_id == row_id + 8 * g, 1.0, 0.0) for g in range(ng)]
    for b in range(NB // step):
        g0 = b * q
        c0 = b * step
        last = b == NB // step - 1
        e = [[_lane_bcast(x[g0 + s], c0 + t) if 8 * (s + 1) > t else None for s in range(q)] for t in range(step)]
        p = None
        if not last:
            p = [[_lane_bcast(x[g0 + q + s], c0 + t) for s in range(q)] for t in range(step)]
        rr = [None] * q
        ss = [None] * q
        rows = []
        for t in range(step):
            gt, st = t // 8, t % 8
            d = _sub_bcast(e[t][gt], st)
            r = lax.rsqrt(d)
            col = [e[t][s] * r if s >= gt else None for s in range(q)]
            rt = _sub_bcast(x[g0 + gt], st) * r
            sr = _sub_bcast(y[g0 + gt], st) * r
            rows.append((rt, sr))
            if st == 0:
                rr[gt], ss[gt] = rt, sr
            else:
                rr[gt] = jnp.where(row_id == st, rt, rr[gt])
                ss[gt] = jnp.where(row_id == st, sr, ss[gt])
            for s in range(gt, q):
                x[g0 + s] = x[g0 + s] - col[s] * rt
                y[g0 + s] = y[g0 + s] - col[s] * sr
            pc = None
            if not last:
                pc = [p[t][s] * r for s in range(q)]
                for s in range(q):
                    x[g0 + q + s] = x[g0 + q + s] - pc[s] * rt
                    y[g0 + q + s] = y[g0 + q + s] - pc[s] * sr
            for u in range(t + 1, step):
                w = _sub_bcast(col[u // 8], u % 8)
                for s in range(u // 8, q):
                    e[u][s] = e[u][s] - col[s] * w
                if not last:
                    for s in range(q):
                        p[u][s] = p[u][s] - pc[s] * w
        for s in range(q):
            store_l(g0 + s, jnp.where(col_id >= row_id + 8 * (g0 + s), rr[s], 0.0))
            store_inv(g0 + s, jnp.where(col_id <= row_id + 8 * (g0 + s), ss[s], 0.0))
        if b < NB // step - 2:
            for s in range(q):
                rt_t = jnp.transpose(rr[s])
                for g in range(g0 + 2 * q, ng):
                    blk = rt_t[8 * g:8 * g + 8, :]
                    for st in range(8):
                        m = jnp.broadcast_to(blk[:, st:st + 1], (8, NB))
                        rt, sr = rows[8 * s + st]
                        x[g] = x[g] - m * rt
                        y[g] = y[g] - m * sr


def dot_nt(a, b):
    return lax.dot_general(a, b, (((1,), (1,)), ((), ())), precision=PREC_HIGH, preferred_element_type=jnp.float32)


def make_kernel(row_procs, col_procs, local_rows, panel_dev):
    steps = panel_dev * col_procs
    row_blocks = local_rows // NB
    slots = panel_dev + 1
    half = row_blocks // 2
    sib_row = CHAIN_ROW ^ 1

    def kernel(pan_in, trl_in, pan_out, trl_out, tile, rowp, colp, linv_in, lnext_in, ldiag_in, stage, win, lwin, linv_c, lt_c, diag,
               in_sem, row_sem, col_sem, linv_sem, lnext_sem, ldiag_sem, win_sem, outc_sem, out_sem,
               row_snd, col_snd, stage_snd, init_snd, linv_snd, lnext_snd, ldiag_snd, give_snd, give_sem):
        pc = lax.axis_index("pc")
        pr = lax.axis_index("pr")
        at_chain_col = pc == CHAIN_COL
        is_chain = jnp.logical_and(at_chain_col, pr == CHAIN_ROW)
        is_sib = jnp.logical_and(at_chain_col, pr == sib_row)
        chain_id = (CHAIN_COL, CHAIN_ROW)
        sib_id = (CHAIN_COL, sib_row)
        some_other = (pc, pr ^ 1)

        def rows(l):
            return pl.ds(pl.multiple_of(l * NB, NB), NB)

        def remote(src, dst, snd, rcv, dev):
            return pltpu.make_async_remote_copy(src_ref=src, dst_ref=dst, send_sem=snd, recv_sem=rcv, device_id=dev, device_id_type=MESH)

        def wait_recv(ref, rcv):
            remote(ref, ref, give_snd.at[0], rcv, some_other).wait_recv()

        barrier = pltpu.get_barrier_semaphore()
        total = row_procs * col_procs
        me = pc * row_procs + pr

        def greet(d, _):
            other = lax.rem(me + d, total)
            pl.semaphore_signal(barrier, inc=1, device_id=(other // row_procs, lax.rem(other, row_procs)), device_id_type=MESH)
            return 0

        def load(m):
            src = pan_in.at[m] if m < panel_dev else trl_in
            return pltpu.make_async_copy(src, tile.at[0, m], in_sem.at[m])

        @pl.when(jnp.logical_not(is_chain))
        def _():
            for m in range(slots):
                load(m).start()

        lax.fori_loop(1, total, greet, 0)
        pl.semaphore_wait(barrier, total - 1)

        def give(m):
            src = pan_in.at[m] if m < panel_dev else trl_in
            return remote(src, tile.at[1, m], give_snd.at[m], give_sem.at[m], sib_id)

        def linv_copy(i, r):
            return remote(linv_c.at[lax.rem(i, RING)], linv_in.at[i // col_procs], linv_snd.at[lax.rem(i, 2), r], linv_sem.at[i // col_procs],
                          (lax.rem(i, col_procs), r))

        def linv_goes(i, r):
            return jnp.logical_or(lax.rem(i, col_procs) != CHAIN_COL, r != CHAIN_ROW)

        def lnext_copy(i, r):
            return remote(lwin.at[lax.rem(i, RING), LAG - 1], lnext_in.at[i // col_procs], lnext_snd.at[lax.rem(i, 2), r],
                          lnext_sem.at[i // col_procs], (lax.rem(i, col_procs), r))

        def ldiag_copy(i):
            return remote(lt_c.at[i], ldiag_in.at[i // col_procs], ldiag_snd.at[lax.rem(i, 2)], ldiag_sem.at[i // col_procs],
                          (lax.rem(i, col_procs), lax.rem(i, row_procs)))

        def drain_chain(i):
            for r in range(row_procs):
                @pl.when(linv_goes(i, r))
                def _():
                    linv_copy(i, r).wait_send()

                    @pl.when(i >= 1)
                    def _():
                        lnext_copy(i, r).wait_send()
            ldiag_copy(i).wait_send()

        def chain_step(i, _):
            for s in range(LAG + 1):
                @pl.when(i - LAG + s >= 0)
                def _():
                    wait_recv(win.at[i, s], win_sem.at[i, s])
            at = lax.rem(i, RING)
            old = [lax.rem(i + RING - LAG + s, RING) for s in range(LAG)]
            for s in range(LAG):
                acc = win[i, s]
                for q in range(s):
                    acc = acc - dot_nt(lwin[at, q], lwin[old[s], LAG - s + q])
                lwin[at, s] = dot_nt(acc, linv_c[old[s]])
            new_diag = win[i, LAG]
            for s in range(LAG):
                new_diag = new_diag - dot_nt(lwin[at, s], lwin[at, s])
            diag[...] = new_diag

            def put_l(g, v):
                lt_c[i, 8 * g:8 * g + 8, :] = v

            def put_inv(g, v):
                linv_c[at, 8 * g:8 * g + 8, :] = v

            chol_inv(lambda g: diag[8 * g:8 * g + 8, :], put_l, put_inv)

            @pl.when(i >= 2)
            def _():
                drain_chain(i - 2)

            for r in range(row_procs):
                @pl.when(linv_goes(i, r))
                def _():
                    linv_copy(i, r).start()

                    @pl.when(i >= 1)
                    def _():
                        lnext_copy(i, r).start()
            ldiag_copy(i).start()
            return 0

        @pl.when(is_chain)
        def _():
            for m in range(slots):
                give(m).start()
            for i in range(RING):
                linv_c[i] = jnp.zeros((NB, NB), jnp.float32)
                for s in range(LAG):
                    lwin[i, s] = jnp.zeros((NB, NB), jnp.float32)
            for i in range(LAG):
                for s in range(LAG - i):
                    win[i, s] = jnp.zeros((NB, NB), jnp.float32)
            lax.fori_loop(0, steps, chain_step, 0)
            drain_chain(steps - 2)
            drain_chain(steps - 1)
            for m in range(slots):
                give(m).wait_send()
            for m in range(slots):
                dst = pan_out.at[m] if m < panel_dev else trl_out
                wait_recv(dst, outc_sem.at[m])

        num_virtual = jnp.where(is_sib, 2, 1)
        col_half = pc // row_procs
        z_me, y_me = pc // 2, lax.rem(pc, 2)
        is_col_src = pr == lax.rem(pc, row_procs)

        def row_of(v):
            return jnp.where(v == 0, pr, CHAIN_ROW)

        def first_block(k, r):
            return (k - r + row_procs) // row_procs

        def row_children(k):
            owner = lax.rem(k, col_procs)
            z_own, y_own = owner // 2, lax.rem(owner, 2)
            to_y = pc == owner
            to_up = jnp.logical_and(z_me >= z_own, z_me < col_procs // 2 - 1)
            to_down = jnp.logical_and(z_me <= z_own, z_me > 0)
            return ((to_y, z_me * 2 + 1 - y_me), (to_up, pc + 2), (to_down, pc - 2))

        def row_copy(k, v, l, c, peer):
            r = row_of(v)
            moved = jnp.logical_and(peer == CHAIN_COL, r == CHAIN_ROW)
            v_dst = jnp.where(moved, 1, 0)
            r_dst = jnp.where(moved, sib_row, r)
            return remote(rowp.at[v, k, rows(l)], rowp.at[v_dst, k, rows(l)], row_snd.at[lax.rem(k, 3), v, l, c],
                          row_sem.at[v_dst, k, l], (peer, r_dst))

        def col_copy(k, v, l, m, d):
            return remote(rowp.at[v, k, rows(l)], colp.at[k, rows(m)], col_snd.at[lax.rem(k, 3), m, d - 1],
                          col_sem.at[k, m], (pc, lax.rem(pr + d, row_procs)))

        def col_goes(d):
            return jnp.logical_not(jnp.logical_and(at_chain_col, lax.rem(pr + d, row_procs) == CHAIN_ROW))

        def needs_col(k, col_block):
            return jnp.logical_and(col_block > k, jnp.logical_or(col_block != k + 1, col_block >= steps))

        def is_col_block(k, v, l):
            here = jnp.logical_and(row_of(v) == lax.rem(pc, row_procs), lax.rem(l, 2) == col_half)
            return jnp.logical_and(here, needs_col(k, pc + (l // 2) * col_procs))

        def each_block(k, act):
            def virtual(v, _):
                def block(l, _):
                    act(v, l)
                    return 0
                return lax.fori_loop(first_block(k, row_of(v)), row_blocks, block, 0)
            lax.fori_loop(0, num_virtual, virtual, 0)

        def each_send(k, v, l, act):
            for c, (goes, peer) in enumerate(row_children(k)):
                @pl.when(goes)
                def _():
                    act(row_copy(k, v, l, c, peer))

            @pl.when(is_col_block(k, v, l))
            def _():
                for d in range(1, row_procs):
                    @pl.when(col_goes(d))
                    def _():
                        act(col_copy(k, v, l, l // 2, d))

        def drain_sends(k):
            each_block(k, lambda v, l: each_send(k, v, l, lambda c: c.wait_send()))

        def stage_copy(v, i, s):
            return remote(stage.at[v, i // row_procs], win.at[i, s], stage_snd.at[v, i // row_procs], win_sem.at[i, s], chain_id)

        def entering(k, v):
            i = k + LAG + 1
            s = lax.rem(pc - (k + 1) + 4 * col_procs, col_procs)
            here = jnp.logical_and(jnp.logical_and(i < steps, s <= LAG), row_of(v) == lax.rem(i, row_procs))
            return here, i, s, (k + 1 + s) // col_procs

        def init_copy(i):
            return remote(pan_in.at[0, pl.ds((i // row_procs) * NB, NB)], win.at[i, jnp.clip(pc - i + LAG, 0, LAG)], init_snd.at[i],
                          win_sem.at[i, jnp.clip(pc - i + LAG, 0, LAG)], chain_id)

        def init_goes(i):
            return jnp.logical_and(pr == i % row_procs, pc <= i)

        def out_local(m):
            dst = pan_out.at[m] if m < panel_dev else trl_out
            return pltpu.make_async_copy(tile.at[0, m], dst, out_sem.at[m])

        def out_remote(m):
            dst = pan_out.at[m] if m < panel_dev else trl_out
            return remote(tile.at[1, m], dst, out_sem.at[slots + m], outc_sem.at[m], chain_id)

        def start_out(m):
            out_local(m).start()

            @pl.when(is_sib)
            def _():
                out_remote(m).start()

        has_src = jnp.logical_or(is_col_src, jnp.logical_and(is_sib, CHAIN_ROW == lax.rem(pc, row_procs)))

        def wait_col(k, m):
            wait_recv(colp.at[k, rows(m)], col_sem.at[k, m])

        def entered_slot(k):
            slot = jnp.int32(-1)
            for v in range(2):
                here, i, s, m = entering(k, v)
                here = jnp.logical_and(jnp.logical_and(here, s > 0), jnp.logical_and(v < num_virtual, k >= 0))
                slot = jnp.where(here, m, slot)
            return slot

        def send_block(k, v, l):
            each_send(k, v, l, lambda c: c.start())

            @pl.when(is_col_block(k, v, l))
            def _():
                colp[k, rows(l // 2), :] = rowp[v, k, rows(l), :]

        def enter(k, v):
            here, i, s, m = entering(k, v)

            @pl.when(jnp.logical_and(here, s > 0))
            def _():
                @pl.when(jnp.logical_not(has_src))
                def _():
                    wait_col(k, m)

                l = i // row_procs
                new = tile[v, m, rows(l), :] - dot_nt(rowp[v, k, rows(l), :], colp[k, rows(m), :])
                tile[v, m, rows(l), :] = new
                stage[v, l] = new
                stage_copy(v, i, s).start()

        def solve_next(k, v, l, first):
            m = (k + 1) // col_procs
            i = row_procs * l + row_of(v)
            new = tile[v, m, rows(l), :]
            if not first:
                prev = jnp.maximum(k - 1, 0)
                old = dot_nt(rowp[v, prev, rows(l), :], colp[prev, rows(m), :])
                skip = jnp.logical_or(k == 0, jnp.logical_and(i == k + LAG, i < steps))
                new = new - jnp.where(skip, 0.0, old)
                new = new - dot_nt(rowp[v, k, rows(l), :], lnext_in[m])

                @pl.when(jnp.logical_and(i == k + LAG + 1, i < steps))
                def _():
                    stage[v, l] = new
                    stage_copy(v, i, 0).start()
            x = dot_nt(new, linv_in[m])
            rowp[v, k + 1, rows(l), :] = x
            tile[v, m, rows(l), :] = x
            send_block(k + 1, v, l)

        def update_row(q, v, l):
            r = row_of(v)
            i_row = row_procs * l + r
            upd = dot_nt(rowp[v, q, rows(l), :], colp[q])
            entered = jnp.logical_and(i_row == q + LAG + 1, i_row < steps)
            for m in range(slots):
                col_block = pc + m * col_procs
                take = jnp.logical_and(col_block > q, jnp.logical_or(col_block > q + 2, col_block >= steps))
                take = jnp.logical_and(take, jnp.logical_not(jnp.logical_and(entered, col_block <= i_row)))
                if m < panel_dev:
                    take = jnp.logical_and(take, i_row >= col_block)

                @pl.when(take)
                def _():
                    tile[v, m, rows(l), :] = tile[v, m, rows(l), :] - upd[:, m * NB:(m + 1) * NB]

        def owner_step(k, _):
            own = jnp.logical_and(pc == lax.rem(k, col_procs), k < steps)
            own_next = jnp.logical_and(pc == lax.rem(k + 1, col_procs), k + 1 < steps)
            m_own = k // col_procs
            m_next = (k + 1) // col_procs
            entered_before = entered_slot(k - 1)

            @pl.when(k >= 2)
            def _():
                drain_sends(k - 2)

            @pl.when(own_next)
            def _():
                wait_recv(linv_in.at[m_next], linv_sem.at[m_next])
                wait_recv(lnext_in.at[m_next], lnext_sem.at[m_next])

                @pl.when(jnp.logical_and(jnp.logical_not(has_src), jnp.logical_and(k >= 1, entered_before != m_next)))
                def _():
                    wait_col(k - 1, m_next)

            def row(t, _):
                @pl.when(jnp.logical_and(t == 2, k >= 1))
                def _():
                    for m in range(slots):
                        col_block = pc + m * col_procs
                        due = jnp.logical_and(needs_col(k - 1, col_block), entered_before != m)
                        due = jnp.logical_and(due, jnp.logical_not(jnp.logical_and(own_next, m == m_next)))

                        @pl.when(jnp.logical_and(due, jnp.logical_not(has_src)))
                        def _():
                            wait_col(k - 1, m)

                def virtual(v, _):
                    r = row_of(v)
                    l = k // row_procs + t

                    @pl.when(jnp.logical_and(jnp.logical_and(l < row_blocks, l >= first_block(k, r)), k < steps))
                    def _():
                        @pl.when(jnp.logical_not(own))
                        def _():
                            wait_recv(rowp.at[v, k, rows(l)], row_sem.at[v, k, l])
                            send_block(k, v, l)

                        @pl.when(jnp.logical_and(own_next, row_procs * l + r > k + 1))
                        def _():
                            solve_next(k, v, l, False)

                    l_upd = l - 2

                    @pl.when(jnp.logical_and(jnp.logical_and(t >= 2, k >= 1), l_upd >= first_block(k - 1, r)))
                    def _():
                        update_row(k - 1, v, l_upd)
                    return 0

                return lax.fori_loop(0, num_virtual, virtual, 0)

            lax.fori_loop(0, row_blocks + 2 - k // row_procs, row, 0)

            def end_of_row(v, _):
                @pl.when(k < steps)
                def _():
                    enter(k, v)
                return 0

            lax.fori_loop(0, num_virtual, end_of_row, 0)

            @pl.when(own)
            def _():
                def finish(v, _):
                    r = row_of(v)

                    @pl.when(r == lax.rem(k, row_procs))
                    def _():
                        wait_recv(ldiag_in.at[m_own], ldiag_sem.at[m_own])
                        tile[v, m_own, rows(k // row_procs), :] = jnp.transpose(ldiag_in[m_own])

                    def clear(l, _):
                        tile[v, m_own, rows(l), :] = jnp.zeros((NB, NB), jnp.float32)
                        return 0

                    lax.fori_loop(0, (k - r + row_procs - 1) // row_procs, clear, 0)
                    return 0

                lax.fori_loop(0, num_virtual, finish, 0)
                for m in range(panel_dev):
                    @pl.when(m_own == m)
                    def _():
                        start_out(m)
            return 0

        def first_column():
            wait_recv(linv_in.at[0], linv_sem.at[0])

            def virtual(v, _):
                def block(l, _):
                    solve_next(-1, v, l, True)
                    return 0
                return lax.fori_loop(first_block(0, row_of(v)), row_blocks, block, 0)
            lax.fori_loop(0, num_virtual, virtual, 0)

        @pl.when(jnp.logical_not(is_chain))
        def _():
            for i in range(LAG + 1):
                @pl.when(init_goes(i))
                def _():
                    init_copy(i).start()
            for m in range(slots):
                load(m).wait()

            @pl.when(is_sib)
            def _():
                for m in range(slots):
                    wait_recv(tile.at[1, m], give_sem.at[m])

            @pl.when(pc == 0)
            def _():
                first_column()

            lax.fori_loop(0, steps + 1, owner_step, 0)
            start_out(panel_dev)
            drain_sends(steps - 1)
            for i in range(LAG + 1):
                @pl.when(init_goes(i))
                def _():
                    init_copy(i).wait_send()

            def drain_stage(k, _):
                def virtual(v, _):
                    here, i, s, m = entering(k, v)

                    @pl.when(here)
                    def _():
                        stage_copy(v, i, s).wait_send()
                    return 0
                return lax.fori_loop(0, num_virtual, virtual, 0)

            lax.fori_loop(0, steps, drain_stage, 0)
            for m in range(slots):
                out_local(m).wait()

                @pl.when(is_sib)
                def _():
                    out_remote(m).wait_send()

    return kernel


def solution(mesh):
    row_procs = mesh.shape["pr"]
    col_procs = mesh.shape["pc"]

    def local_part(panel_tile, trail_tile):
        local_rows, panel_dev, _ = panel_tile.shape
        steps = panel_dev * col_procs
        row_blocks = local_rows // NB
        slots = panel_dev + 1
        f32 = jnp.float32
        dma = pltpu.SemaphoreType.DMA
        scratch = [
            pltpu.VMEM((2, slots, local_rows, NB), f32),
            pltpu.VMEM((2, steps, local_rows, NB), f32),
            pltpu.VMEM((steps, slots * NB, NB), f32),
            pltpu.VMEM((panel_dev, NB, NB), f32),
            pltpu.VMEM((panel_dev, NB, NB), f32),
            pltpu.VMEM((panel_dev, NB, NB), f32),
            pltpu.VMEM((2, steps // row_procs, NB, NB), f32),
            pltpu.VMEM((steps, LAG + 1, NB, NB), f32),
            pltpu.VMEM((RING, LAG, NB, NB), f32),
            pltpu.VMEM((RING, NB, NB), f32),
            pltpu.VMEM((steps, NB, NB), f32),
            pltpu.VMEM((NB, NB), f32),
            dma((slots,)),
            dma((2, steps, row_blocks)),
            dma((steps, slots)),
            dma((panel_dev,)),
            dma((panel_dev,)),
            dma((panel_dev,)),
            dma((steps, LAG + 1)),
            dma((slots,)),
            dma((2 * slots,)),
            dma((3, 2, row_blocks, 3)),
            dma((3, slots, row_procs - 1)),
            dma((2, steps // row_procs)),
            dma((LAG + 1,)),
            dma((2, row_procs)),
            dma((2, row_procs)),
            dma((2,)),
            dma((slots,)),
            dma((slots,)),
        ]
        hbm = pl.BlockSpec(memory_space=pl.ANY)
        by_slot = jnp.transpose(panel_tile, (1, 0, 2))
        panel_new, trail_new = pl.pallas_call(
            make_kernel(row_procs, col_procs, local_rows, panel_dev),
            out_shape=[jax.ShapeDtypeStruct(by_slot.shape, f32), jax.ShapeDtypeStruct(trail_tile.shape, f32)],
            in_specs=[hbm, hbm],
            out_specs=[hbm, hbm],
            scratch_shapes=scratch,
            compiler_params=pltpu.CompilerParams(collective_id=0, has_side_effects=True, vmem_limit_bytes=67043328),
        )(by_slot, trail_tile)
        return jnp.transpose(panel_new, (1, 0, 2)), trail_new

    spec_panel = P("pr", "pc", None)
    spec_trail = P("pr", "pc")
    return jax.shard_map(local_part, mesh=mesh, in_specs=(spec_panel, spec_trail), out_specs=(spec_panel, spec_trail), check_vma=False)
```

```python
import jax
import jax.numpy as jnp
from jax import lax
from jax.experimental import pallas as pl
from jax.experimental.pallas import tpu as pltpu
from jax.sharding import PartitionSpec as P

MESH = pl.DeviceIdType.MESH
PREC_HIGH = lax.Precision.HIGHEST
NB = 128
LAG = 3
CHAIN_COL = 2
CHAIN_ROW = 1
RING = 8


def _sub_bcast(v, s):
    return jnp.broadcast_to(v[s:s + 1, :], (8, NB))


def _lane_bcast(v, c):
    return jnp.broadcast_to(v[:, c:c + 1], (8, NB))


def chol_inv(load, store_l, store_inv, q=2):
    ng = NB // 8
    step = 8 * q
    x = [load(g) for g in range(ng)]
    row_id = lax.broadcasted_iota(jnp.int32, (8, NB), 0)
    col_id = lax.broadcasted_iota(jnp.int32, (8, NB), 1)
    y = [jnp.where(col_id == row_id + 8 * g, 1.0, 0.0) for g in range(ng)]
    for b in range(NB // step):
        g0 = b * q
        c0 = b * step
        last = b == NB // step - 1
        e = [[_lane_bcast(x[g0 + s], c0 + t) if 8 * (s + 1) > t else None for s in range(q)] for t in range(step)]
        p = None
        if not last:
            p = [[_lane_bcast(x[g0 + q + s], c0 + t) for s in range(q)] for t in range(step)]
        rr = [None] * q
        ss = [None] * q
        rows = []
        for t in range(step):
            gt, st = t // 8, t % 8
            d = _sub_bcast(e[t][gt], st)
            r = lax.rsqrt(d)
            col = [e[t][s] * r if s >= gt else None for s in range(q)]
            rt = _sub_bcast(x[g0 + gt], st) * r
            sr = _sub_bcast(y[g0 + gt], st) * r
            rows.append((rt, sr))
            if st == 0:
                rr[gt], ss[gt] = rt, sr
            else:
                rr[gt] = jnp.where(row_id == st, rt, rr[gt])
                ss[gt] = jnp.where(row_id == st, sr, ss[gt])
            for s in range(gt, q):
                x[g0 + s] = x[g0 + s] - col[s] * rt
                y[g0 + s] = y[g0 + s] - col[s] * sr
            pc = None
            if not last:
                pc = [p[t][s] * r for s in range(q)]
                for s in range(q):
                    x[g0 + q + s] = x[g0 + q + s] - pc[s] * rt
                    y[g0 + q + s] = y[g0 + q + s] - pc[s] * sr
            for u in range(t + 1, step):
                w = _sub_bcast(col[u // 8], u % 8)
                for s in range(u // 8, q):
                    e[u][s] = e[u][s] - col[s] * w
                if not last:
                    for s in range(q):
                        p[u][s] = p[u][s] - pc[s] * w
        for s in range(q):
            store_l(g0 + s, jnp.where(col_id >= row_id + 8 * (g0 + s), rr[s], 0.0))
            store_inv(g0 + s, jnp.where(col_id <= row_id + 8 * (g0 + s), ss[s], 0.0))
        if b < NB // step - 2:
            for s in range(q):
                rt_t = jnp.transpose(rr[s])
                for g in range(g0 + 2 * q, ng):
                    blk = rt_t[8 * g:8 * g + 8, :]
                    for st in range(8):
                        m = jnp.broadcast_to(blk[:, st:st + 1], (8, NB))
                        rt, sr = rows[8 * s + st]
                        x[g] = x[g] - m * rt
                        y[g] = y[g] - m * sr


def dot_nt(a, b):
    return lax.dot_general(a, b, (((1,), (1,)), ((), ())), precision=PREC_HIGH, preferred_element_type=jnp.float32)


def make_kernel(row_procs, col_procs, local_rows, panel_dev):
    steps = panel_dev * col_procs
    row_blocks = local_rows // NB
    slots = panel_dev + 1
    half = row_blocks // 2
    sib_row = CHAIN_ROW ^ 1

    def kernel(pan_in, trl_in, pan_out, trl_out, tile, rowp, colp, linv_in, lnext_in, ldiag_in, stage, win, lwin, linv_c, lt_c, diag,
               in_sem, row_sem, col_sem, linv_sem, lnext_sem, ldiag_sem, win_sem, outc_sem, out_sem,
               row_snd, col_snd, stage_snd, init_snd, linv_snd, lnext_snd, ldiag_snd, give_snd, give_sem):
        pc = lax.axis_index("pc")
        pr = lax.axis_index("pr")
        at_chain_col = pc == CHAIN_COL
        is_chain = jnp.logical_and(at_chain_col, pr == CHAIN_ROW)
        is_sib = jnp.logical_and(at_chain_col, pr == sib_row)
        chain_id = (CHAIN_COL, CHAIN_ROW)
        sib_id = (CHAIN_COL, sib_row)
        some_other = (pc, pr ^ 1)

        def rows(l):
            return pl.ds(pl.multiple_of(l * NB, NB), NB)

        def remote(src, dst, snd, rcv, dev):
            return pltpu.make_async_remote_copy(src_ref=src, dst_ref=dst, send_sem=snd, recv_sem=rcv, device_id=dev, device_id_type=MESH)

        def wait_recv(ref, rcv):
            remote(ref, ref, give_snd.at[0], rcv, some_other).wait_recv()

        barrier = pltpu.get_barrier_semaphore()
        total = row_procs * col_procs
        me = pc * row_procs + pr

        def greet(d, _):
            other = lax.rem(me + d, total)
            pl.semaphore_signal(barrier, inc=1, device_id=(other // row_procs, lax.rem(other, row_procs)), device_id_type=MESH)
            return 0

        def load(m):
            src = pan_in.at[m] if m < panel_dev else trl_in
            return pltpu.make_async_copy(src, tile.at[0, m], in_sem.at[m])

        @pl.when(jnp.logical_not(is_chain))
        def _():
            for m in range(slots):
                load(m).start()

        lax.fori_loop(1, total, greet, 0)
        pl.semaphore_wait(barrier, total - 1)

        def give(m):
            src = pan_in.at[m] if m < panel_dev else trl_in
            return remote(src, tile.at[1, m], give_snd.at[m], give_sem.at[m], sib_id)

        def linv_copy(i, r):
            return remote(linv_c.at[lax.rem(i, RING)], linv_in.at[i // col_procs], linv_snd.at[lax.rem(i, 2), r], linv_sem.at[i // col_procs],
                          (lax.rem(i, col_procs), r))

        def linv_goes(i, r):
            return jnp.logical_or(lax.rem(i, col_procs) != CHAIN_COL, r != CHAIN_ROW)

        def lnext_copy(i, r):
            return remote(lwin.at[lax.rem(i, RING), LAG - 1], lnext_in.at[i // col_procs], lnext_snd.at[lax.rem(i, 2), r],
                          lnext_sem.at[i // col_procs], (lax.rem(i, col_procs), r))

        def ldiag_copy(i):
            return remote(lt_c.at[i], ldiag_in.at[i // col_procs], ldiag_snd.at[lax.rem(i, 2)], ldiag_sem.at[i // col_procs],
                          (lax.rem(i, col_procs), lax.rem(i, row_procs)))

        def drain_chain(i):
            for r in range(row_procs):
                @pl.when(linv_goes(i, r))
                def _():
                    linv_copy(i, r).wait_send()

                    @pl.when(i >= 1)
                    def _():
                        lnext_copy(i, r).wait_send()
            ldiag_copy(i).wait_send()

        def chain_step(i, _):
            for s in range(LAG + 1):
                @pl.when(i - LAG + s >= 0)
                def _():
                    wait_recv(win.at[i, s], win_sem.at[i, s])
            at = lax.rem(i, RING)
            old = [lax.rem(i + RING - LAG + s, RING) for s in range(LAG)]
            for s in range(LAG):
                acc = win[i, s]
                for q in range(s):
                    acc = acc - dot_nt(lwin[at, q], lwin[old[s], LAG - s + q])
                lwin[at, s] = dot_nt(acc, linv_c[old[s]])
            new_diag = win[i, LAG]
            for s in range(LAG):
                new_diag = new_diag - dot_nt(lwin[at, s], lwin[at, s])
            diag[...] = new_diag

            def put_l(g, v):
                lt_c[i, 8 * g:8 * g + 8, :] = v

            def put_inv(g, v):
                linv_c[at, 8 * g:8 * g + 8, :] = v

            chol_inv(lambda g: diag[8 * g:8 * g + 8, :], put_l, put_inv)

            @pl.when(i >= 2)
            def _():
                drain_chain(i - 2)

            for r in range(row_procs):
                @pl.when(linv_goes(i, r))
                def _():
                    linv_copy(i, r).start()

                    @pl.when(i >= 1)
                    def _():
                        lnext_copy(i, r).start()
            ldiag_copy(i).start()
            return 0

        @pl.when(is_chain)
        def _():
            for m in range(slots):
                give(m).start()
            for i in range(RING):
                linv_c[i] = jnp.zeros((NB, NB), jnp.float32)
                for s in range(LAG):
                    lwin[i, s] = jnp.zeros((NB, NB), jnp.float32)
            for i in range(LAG):
                for s in range(LAG - i):
                    win[i, s] = jnp.zeros((NB, NB), jnp.float32)
            lax.fori_loop(0, steps, chain_step, 0)
            drain_chain(steps - 2)
            drain_chain(steps - 1)
            for m in range(slots):
                give(m).wait_send()
            for m in range(slots):
                dst = pan_out.at[m] if m < panel_dev else trl_out
                wait_recv(dst, outc_sem.at[m])

        num_virtual = jnp.where(is_sib, 2, 1)
        col_half = pc // row_procs
        z_me, y_me = pc // 2, lax.rem(pc, 2)
        is_col_src = pr == lax.rem(pc, row_procs)

        def row_of(v):
            return jnp.where(v == 0, pr, CHAIN_ROW)

        def first_block(k, r):
            return (k - r + row_procs) // row_procs

        def row_children(k):
            owner = lax.rem(k, col_procs)
            follows = jnp.where(k + 1 < steps, lax.rem(k + 1, col_procs), -1)
            z_own, y_own = owner // 2, lax.rem(owner, 2)
            y_far = 1 - y_own
            z_by = jnp.where(z_own < col_procs // 2 - 1, z_own + 1, z_own - 1)

            def parents(peer):
                z, y = peer // 2, lax.rem(peer, 2)
                inward = jnp.where(z < z_own, z + 1, z - 1)
                in_line = y == y_own
                even = jnp.where(in_line, inward * 2 + y, jnp.where(z == z_own, z_by * 2 + y, z * 2 + y_own))
                odd = jnp.where(in_line, z * 2 + y_far, jnp.where(z == z_own, owner, inward * 2 + y))
                first = peer == follows
                return jnp.where(first, owner, even), jnp.where(first, owner, odd)

            found = []
            for peer, valid in ((z_me * 2 + 1 - y_me, True), (pc + 2, z_me < col_procs // 2 - 1), (pc - 2, z_me > 0)):
                ok = jnp.logical_and(valid, peer != owner)
                even, odd = parents(jnp.maximum(peer, 0))
                found.append((jnp.logical_and(ok, even == pc), jnp.logical_and(ok, odd == pc), peer))
            jump = jnp.logical_and(jnp.logical_and(pc == owner, y_own == 1), follows >= 0)
            found.append((jump, jump, jnp.maximum(follows, 0)))
            return found

        def row_copy(k, v, l, c, peer):
            r = row_of(v)
            moved = jnp.logical_and(peer == CHAIN_COL, r == CHAIN_ROW)
            v_dst = jnp.where(moved, 1, 0)
            r_dst = jnp.where(moved, sib_row, r)
            return remote(rowp.at[v, k, rows(l)], rowp.at[v_dst, k, rows(l)], row_snd.at[lax.rem(k, 3), v, l, c],
                          row_sem.at[v_dst, k, l], (peer, r_dst))

        def col_copy(k, v, l, m, d):
            return remote(rowp.at[v, k, rows(l)], colp.at[k, rows(m)], col_snd.at[lax.rem(k, 3), m, d - 1],
                          col_sem.at[k, m], (pc, lax.rem(pr + d, row_procs)))

        def col_goes(d):
            return jnp.logical_not(jnp.logical_and(at_chain_col, lax.rem(pr + d, row_procs) == CHAIN_ROW))

        def needs_col(k, col_block):
            return jnp.logical_and(col_block > k, jnp.logical_or(col_block != k + 1, col_block >= steps))

        def is_col_block(k, v, l):
            here = jnp.logical_and(row_of(v) == lax.rem(pc, row_procs), lax.rem(l, 2) == col_half)
            return jnp.logical_and(here, needs_col(k, pc + (l // 2) * col_procs))

        def each_block(k, act):
            def virtual(v, _):
                def block(l, _):
                    act(v, l)
                    return 0
                return lax.fori_loop(first_block(k, row_of(v)), row_blocks, block, 0)
            lax.fori_loop(0, num_virtual, virtual, 0)

        def each_send(k, v, l, act, children):
            odd_row = lax.rem(l, 2) == 1
            for c, (even, odd, peer) in enumerate(children):
                @pl.when(jnp.where(odd_row, odd, even))
                def _():
                    act(row_copy(k, v, l, c, peer))

            @pl.when(is_col_block(k, v, l))
            def _():
                for d in range(1, row_procs):
                    @pl.when(col_goes(d))
                    def _():
                        act(col_copy(k, v, l, l // 2, d))

        def drain_sends(k):
            children = row_children(k)
            each_block(k, lambda v, l: each_send(k, v, l, lambda c: c.wait_send(), children))

        def stage_copy(v, i, s):
            return remote(stage.at[v, i // row_procs], win.at[i, s], stage_snd.at[v, i // row_procs], win_sem.at[i, s], chain_id)

        def entering(k, v):
            i = k + LAG + 1
            s = lax.rem(pc - (k + 1) + 4 * col_procs, col_procs)
            here = jnp.logical_and(jnp.logical_and(i < steps, s <= LAG), row_of(v) == lax.rem(i, row_procs))
            return here, i, s, (k + 1 + s) // col_procs

        def init_copy(i):
            return remote(pan_in.at[0, pl.ds((i // row_procs) * NB, NB)], win.at[i, jnp.clip(pc - i + LAG, 0, LAG)], init_snd.at[i],
                          win_sem.at[i, jnp.clip(pc - i + LAG, 0, LAG)], chain_id)

        def init_goes(i):
            return jnp.logical_and(pr == i % row_procs, pc <= i)

        def out_local(m):
            dst = pan_out.at[m] if m < panel_dev else trl_out
            return pltpu.make_async_copy(tile.at[0, m], dst, out_sem.at[m])

        def out_remote(m):
            dst = pan_out.at[m] if m < panel_dev else trl_out
            return remote(tile.at[1, m], dst, out_sem.at[slots + m], outc_sem.at[m], chain_id)

        def start_out(m):
            out_local(m).start()

            @pl.when(is_sib)
            def _():
                out_remote(m).start()

        has_src = jnp.logical_or(is_col_src, jnp.logical_and(is_sib, CHAIN_ROW == lax.rem(pc, row_procs)))

        def wait_col(k, m):
            wait_recv(colp.at[k, rows(m)], col_sem.at[k, m])

        def entered_slot(k):
            slot = jnp.int32(-1)
            for v in range(2):
                here, i, s, m = entering(k, v)
                here = jnp.logical_and(jnp.logical_and(here, s > 0), jnp.logical_and(v < num_virtual, k >= 0))
                slot = jnp.where(here, m, slot)
            return slot

        def send_block(k, v, l, children):
            each_send(k, v, l, lambda c: c.start(), children)

            @pl.when(is_col_block(k, v, l))
            def _():
                colp[k, rows(l // 2), :] = rowp[v, k, rows(l), :]

        def enter(k, v):
            here, i, s, m = entering(k, v)

            @pl.when(jnp.logical_and(here, s > 0))
            def _():
                @pl.when(jnp.logical_not(has_src))
                def _():
                    wait_col(k, m)

                l = i // row_procs
                new = tile[v, m, rows(l), :] - dot_nt(rowp[v, k, rows(l), :], colp[k, rows(m), :])
                tile[v, m, rows(l), :] = new
                stage[v, l] = new
                stage_copy(v, i, s).start()

        def solve_next(k, v, l, first, children):
            m = (k + 1) // col_procs
            i = row_procs * l + row_of(v)
            new = tile[v, m, rows(l), :]
            if not first:
                prev = jnp.maximum(k - 1, 0)
                skip = jnp.logical_or(k == 0, jnp.logical_and(i == k + LAG, i < steps))
                left = jnp.concatenate([jnp.where(skip, 0.0, rowp[v, prev, rows(l), :]), rowp[v, k, rows(l), :]], axis=1)
                right = jnp.concatenate([jnp.where(k == 0, 0.0, colp[prev, rows(m), :]), lnext_in[m]], axis=1)
                new = new - dot_nt(left, right)

                @pl.when(jnp.logical_and(i == k + LAG + 1, i < steps))
                def _():
                    stage[v, l] = new
                    stage_copy(v, i, 0).start()
            x = dot_nt(new, linv_in[m])
            rowp[v, k + 1, rows(l), :] = x
            tile[v, m, rows(l), :] = x
            send_block(k + 1, v, l, children)

        def update_row(q, v, l):
            r = row_of(v)
            i_row = row_procs * l + r
            upd = dot_nt(rowp[v, q, rows(l), :], colp[q])
            entered = jnp.logical_and(i_row == q + LAG + 1, i_row < steps)
            for m in range(slots):
                col_block = pc + m * col_procs
                take = jnp.logical_and(col_block > q, jnp.logical_or(col_block > q + 2, col_block >= steps))
                take = jnp.logical_and(take, jnp.logical_not(jnp.logical_and(entered, col_block <= i_row)))
                if m < panel_dev:
                    take = jnp.logical_and(take, i_row >= col_block)

                @pl.when(take)
                def _():
                    tile[v, m, rows(l), :] = tile[v, m, rows(l), :] - upd[:, m * NB:(m + 1) * NB]

        def owner_step(k, _):
            own = jnp.logical_and(pc == lax.rem(k, col_procs), k < steps)
            own_next = jnp.logical_and(pc == lax.rem(k + 1, col_procs), k + 1 < steps)
            m_own = k // col_procs
            m_next = (k + 1) // col_procs
            entered_before = entered_slot(k - 1)
            children = row_children(k)
            children_next = row_children(k + 1)

            @pl.when(k >= 2)
            def _():
                drain_sends(k - 2)

            @pl.when(own_next)
            def _():
                wait_recv(linv_in.at[m_next], linv_sem.at[m_next])
                wait_recv(lnext_in.at[m_next], lnext_sem.at[m_next])

                @pl.when(jnp.logical_and(jnp.logical_not(has_src), jnp.logical_and(k >= 1, entered_before != m_next)))
                def _():
                    wait_col(k - 1, m_next)

            def row(t, _):
                @pl.when(jnp.logical_and(t == 2, k >= 1))
                def _():
                    for m in range(slots):
                        col_block = pc + m * col_procs
                        due = jnp.logical_and(needs_col(k - 1, col_block), entered_before != m)
                        due = jnp.logical_and(due, jnp.logical_not(jnp.logical_and(own_next, m == m_next)))

                        @pl.when(jnp.logical_and(due, jnp.logical_not(has_src)))
                        def _():
                            wait_col(k - 1, m)

                def virtual(v, _):
                    r = row_of(v)
                    l = k // row_procs + t

                    @pl.when(jnp.logical_and(jnp.logical_and(l < row_blocks, l >= first_block(k, r)), k < steps))
                    def _():
                        @pl.when(jnp.logical_not(own))
                        def _():
                            wait_recv(rowp.at[v, k, rows(l)], row_sem.at[v, k, l])
                            send_block(k, v, l, children)

                        @pl.when(jnp.logical_and(own_next, row_procs * l + r > k + 1))
                        def _():
                            solve_next(k, v, l, False, children_next)

                    l_upd = l - 2

                    @pl.when(jnp.logical_and(jnp.logical_and(t >= 2, k >= 1), l_upd >= first_block(k - 1, r)))
                    def _():
                        update_row(k - 1, v, l_upd)
                    return 0

                return lax.fori_loop(0, num_virtual, virtual, 0)

            lax.fori_loop(0, row_blocks + 2 - k // row_procs, row, 0)

            def end_of_row(v, _):
                @pl.when(k < steps)
                def _():
                    enter(k, v)
                return 0

            lax.fori_loop(0, num_virtual, end_of_row, 0)

            @pl.when(own)
            def _():
                def finish(v, _):
                    r = row_of(v)

                    @pl.when(r == lax.rem(k, row_procs))
                    def _():
                        wait_recv(ldiag_in.at[m_own], ldiag_sem.at[m_own])
                        tile[v, m_own, rows(k // row_procs), :] = jnp.transpose(ldiag_in[m_own])

                    def clear(l, _):
                        tile[v, m_own, rows(l), :] = jnp.zeros((NB, NB), jnp.float32)
                        return 0

                    lax.fori_loop(0, (k - r + row_procs - 1) // row_procs, clear, 0)
                    return 0

                lax.fori_loop(0, num_virtual, finish, 0)
                for m in range(panel_dev):
                    @pl.when(m_own == m)
                    def _():
                        start_out(m)
            return 0

        def first_column():
            wait_recv(linv_in.at[0], linv_sem.at[0])
            children = row_children(0)

            def virtual(v, _):
                def block(l, _):
                    solve_next(-1, v, l, True, children)
                    return 0
                return lax.fori_loop(first_block(0, row_of(v)), row_blocks, block, 0)
            lax.fori_loop(0, num_virtual, virtual, 0)

        @pl.when(jnp.logical_not(is_chain))
        def _():
            for i in range(LAG + 1):
                @pl.when(init_goes(i))
                def _():
                    init_copy(i).start()
            for m in range(slots):
                load(m).wait()

            @pl.when(is_sib)
            def _():
                for m in range(slots):
                    wait_recv(tile.at[1, m], give_sem.at[m])

            @pl.when(pc == 0)
            def _():
                first_column()

            lax.fori_loop(0, steps + 1, owner_step, 0)
            start_out(panel_dev)
            drain_sends(steps - 1)
            for i in range(LAG + 1):
                @pl.when(init_goes(i))
                def _():
                    init_copy(i).wait_send()

            def drain_stage(k, _):
                def virtual(v, _):
                    here, i, s, m = entering(k, v)

                    @pl.when(here)
                    def _():
                        stage_copy(v, i, s).wait_send()
                    return 0
                return lax.fori_loop(0, num_virtual, virtual, 0)

            lax.fori_loop(0, steps, drain_stage, 0)
            for m in range(slots):
                out_local(m).wait()

                @pl.when(is_sib)
                def _():
                    out_remote(m).wait_send()

    return kernel


def solution(mesh):
    row_procs = mesh.shape["pr"]
    col_procs = mesh.shape["pc"]

    def local_part(panel_tile, trail_tile):
        local_rows, panel_dev, _ = panel_tile.shape
        steps = panel_dev * col_procs
        row_blocks = local_rows // NB
        slots = panel_dev + 1
        f32 = jnp.float32
        dma = pltpu.SemaphoreType.DMA
        scratch = [
            pltpu.VMEM((2, slots, local_rows, NB), f32),
            pltpu.VMEM((2, steps, local_rows, NB), f32),
            pltpu.VMEM((steps, slots * NB, NB), f32),
            pltpu.VMEM((panel_dev, NB, NB), f32),
            pltpu.VMEM((panel_dev, NB, NB), f32),
            pltpu.VMEM((panel_dev, NB, NB), f32),
            pltpu.VMEM((2, steps // row_procs, NB, NB), f32),
            pltpu.VMEM((steps, LAG + 1, NB, NB), f32),
            pltpu.VMEM((RING, LAG, NB, NB), f32),
            pltpu.VMEM((RING, NB, NB), f32),
            pltpu.VMEM((steps, NB, NB), f32),
            pltpu.VMEM((NB, NB), f32),
            dma((slots,)),
            dma((2, steps, row_blocks)),
            dma((steps, slots)),
            dma((panel_dev,)),
            dma((panel_dev,)),
            dma((panel_dev,)),
            dma((steps, LAG + 1)),
            dma((slots,)),
            dma((2 * slots,)),
            dma((3, 2, row_blocks, 4)),
            dma((3, slots, row_procs - 1)),
            dma((2, steps // row_procs)),
            dma((LAG + 1,)),
            dma((2, row_procs)),
            dma((2, row_procs)),
            dma((2,)),
            dma((slots,)),
            dma((slots,)),
        ]
        hbm = pl.BlockSpec(memory_space=pl.ANY)
        by_slot = jnp.transpose(panel_tile, (1, 0, 2))
        panel_new, trail_new = pl.pallas_call(
            make_kernel(row_procs, col_procs, local_rows, panel_dev),
            out_shape=[jax.ShapeDtypeStruct(by_slot.shape, f32), jax.ShapeDtypeStruct(trail_tile.shape, f32)],
            in_specs=[hbm, hbm],
            out_specs=[hbm, hbm],
            scratch_shapes=scratch,
            compiler_params=pltpu.CompilerParams(collective_id=0, has_side_effects=True, vmem_limit_bytes=67043328),
        )(by_slot, trail_tile)
        return jnp.transpose(panel_new, (1, 0, 2)), trail_new

    spec_panel = P("pr", "pc", None)
    spec_trail = P("pr", "pc")
    return jax.shard_map(local_part, mesh=mesh, in_specs=(spec_panel, spec_trail), out_specs=(spec_panel, spec_trail), check_vma=False)
```

```python
import jax
import jax.numpy as jnp
from jax import lax
from jax.experimental import pallas as pl
from jax.experimental.pallas import tpu as pltpu
from jax.sharding import PartitionSpec as P

MESH = pl.DeviceIdType.MESH
PREC_HIGH = lax.Precision.HIGHEST
NB = 128
LAG = 4
CHAIN_COL = 2
CHAIN_ROW = 1
RING = 8
BEHIND = 2


def _sub_bcast(v, s):
    return jnp.broadcast_to(v[s:s + 1, :], (8, NB))


def _lane_bcast(v, c):
    return jnp.broadcast_to(v[:, c:c + 1], (8, NB))


def chol_inv(load, store_l, store_inv, q=2):
    ng = NB // 8
    step = 8 * q
    x = [load(g) for g in range(ng)]
    row_id = lax.broadcasted_iota(jnp.int32, (8, NB), 0)
    col_id = lax.broadcasted_iota(jnp.int32, (8, NB), 1)
    y = [jnp.where(col_id == row_id + 8 * g, 1.0, 0.0) for g in range(ng)]
    for b in range(NB // step):
        g0 = b * q
        c0 = b * step
        last = b == NB // step - 1
        e = [[_lane_bcast(x[g0 + s], c0 + t) if 8 * (s + 1) > t else None for s in range(q)] for t in range(step)]
        p = None
        if not last:
            p = [[_lane_bcast(x[g0 + q + s], c0 + t) for s in range(q)] for t in range(step)]
        rr = [None] * q
        ss = [None] * q
        rows = []
        for t in range(step):
            gt, st = t // 8, t % 8
            d = _sub_bcast(e[t][gt], st)
            r = lax.rsqrt(d)
            col = [e[t][s] * r if s >= gt else None for s in range(q)]
            rt = _sub_bcast(x[g0 + gt], st) * r
            sr = _sub_bcast(y[g0 + gt], st) * r
            rows.append((rt, sr))
            if st == 0:
                rr[gt], ss[gt] = rt, sr
            else:
                rr[gt] = jnp.where(row_id == st, rt, rr[gt])
                ss[gt] = jnp.where(row_id == st, sr, ss[gt])
            for s in range(gt, q):
                x[g0 + s] = x[g0 + s] - col[s] * rt
                y[g0 + s] = y[g0 + s] - col[s] * sr
            pc = None
            if not last:
                pc = [p[t][s] * r for s in range(q)]
                for s in range(q):
                    x[g0 + q + s] = x[g0 + q + s] - pc[s] * rt
                    y[g0 + q + s] = y[g0 + q + s] - pc[s] * sr
            for u in range(t + 1, step):
                w = _sub_bcast(col[u // 8], u % 8)
                for s in range(u // 8, q):
                    e[u][s] = e[u][s] - col[s] * w
                if not last:
                    for s in range(q):
                        p[u][s] = p[u][s] - pc[s] * w
        for s in range(q):
            store_l(g0 + s, jnp.where(col_id >= row_id + 8 * (g0 + s), rr[s], 0.0))
            store_inv(g0 + s, jnp.where(col_id <= row_id + 8 * (g0 + s), ss[s], 0.0))
        if b < NB // step - 2:
            for s in range(q):
                rt_t = jnp.transpose(rr[s])
                for g in range(g0 + 2 * q, ng):
                    blk = rt_t[8 * g:8 * g + 8, :]
                    for st in range(8):
                        m = jnp.broadcast_to(blk[:, st:st + 1], (8, NB))
                        rt, sr = rows[8 * s + st]
                        x[g] = x[g] - m * rt
                        y[g] = y[g] - m * sr


def dot_nt(a, b):
    return lax.dot_general(a, b, (((1,), (1,)), ((), ())), precision=PREC_HIGH, preferred_element_type=jnp.float32)


def make_kernel(row_procs, col_procs, local_rows, panel_dev):
    steps = panel_dev * col_procs
    row_blocks = local_rows // NB
    slots = panel_dev + 1
    half = row_blocks // 2
    sib_row = CHAIN_ROW ^ 1

    def kernel(pan_in, trl_in, pan_out, trl_out, tile, rowp, colp, linv_in, lnext_in, ldiag_in, stage, win, lwin, linv_c, lt_c, diag,
               in_sem, row_sem, col_sem, linv_sem, lnext_sem, ldiag_sem, win_sem, outc_sem, out_sem,
               row_snd, col_snd, stage_snd, init_snd, linv_snd, lnext_snd, ldiag_snd, give_snd, give_sem):
        pc = lax.axis_index("pc")
        pr = lax.axis_index("pr")
        at_chain_col = pc == CHAIN_COL
        is_chain = jnp.logical_and(at_chain_col, pr == CHAIN_ROW)
        is_sib = jnp.logical_and(at_chain_col, pr == sib_row)
        chain_id = (CHAIN_COL, CHAIN_ROW)
        sib_id = (CHAIN_COL, sib_row)
        some_other = (pc, pr ^ 1)

        def rows(l):
            return pl.ds(pl.multiple_of(l * NB, NB), NB)

        def remote(src, dst, snd, rcv, dev):
            return pltpu.make_async_remote_copy(src_ref=src, dst_ref=dst, send_sem=snd, recv_sem=rcv, device_id=dev, device_id_type=MESH)

        def wait_recv(ref, rcv):
            remote(ref, ref, give_snd.at[0], rcv, some_other).wait_recv()

        barrier = pltpu.get_barrier_semaphore()
        total = row_procs * col_procs
        me = pc * row_procs + pr

        def greet(d, _):
            other = lax.rem(me + d, total)
            pl.semaphore_signal(barrier, inc=1, device_id=(other // row_procs, lax.rem(other, row_procs)), device_id_type=MESH)
            return 0

        def load(m):
            src = pan_in.at[m] if m < panel_dev else trl_in
            return pltpu.make_async_copy(src, tile.at[0, m], in_sem.at[m])

        @pl.when(jnp.logical_not(is_chain))
        def _():
            for m in range(slots):
                load(m).start()

        lax.fori_loop(1, total, greet, 0)
        pl.semaphore_wait(barrier, total - 1)

        def give(m):
            src = pan_in.at[m] if m < panel_dev else trl_in
            return remote(src, tile.at[1, m], give_snd.at[m], give_sem.at[m], sib_id)

        def linv_copy(i, r):
            return remote(linv_c.at[lax.rem(i, RING)], linv_in.at[i // col_procs], linv_snd.at[lax.rem(i, 2), r], linv_sem.at[i // col_procs],
                          (lax.rem(i, col_procs), r))

        def linv_goes(i, r):
            return jnp.logical_or(lax.rem(i, col_procs) != CHAIN_COL, r != CHAIN_ROW)

        def lnext_copy(i, r):
            return remote(lwin.at[lax.rem(i, RING), LAG - 1], lnext_in.at[i // col_procs], lnext_snd.at[lax.rem(i, 2), r],
                          lnext_sem.at[i // col_procs], (lax.rem(i, col_procs), r))

        def ldiag_copy(i):
            return remote(lt_c.at[i], ldiag_in.at[i // col_procs], ldiag_snd.at[lax.rem(i, 2)], ldiag_sem.at[i // col_procs],
                          (lax.rem(i, col_procs), lax.rem(i, row_procs)))

        def drain_chain(i):
            for r in range(row_procs):
                @pl.when(linv_goes(i, r))
                def _():
                    linv_copy(i, r).wait_send()

                    @pl.when(i >= 1)
                    def _():
                        lnext_copy(i, r).wait_send()
            ldiag_copy(i).wait_send()

        def chain_step(i, _):
            for s in range(LAG + 1):
                @pl.when(i - LAG + s >= 0)
                def _():
                    wait_recv(win.at[i, s], win_sem.at[i, s])
            at = lax.rem(i, RING)
            old = [lax.rem(i + RING - LAG + s, RING) for s in range(LAG)]
            for s in range(LAG):
                acc = win[i, s]
                for q in range(s):
                    acc = acc - dot_nt(lwin[at, q], lwin[old[s], LAG - s + q])
                lwin[at, s] = dot_nt(acc, linv_c[old[s]])
            new_diag = win[i, LAG]
            for s in range(LAG):
                new_diag = new_diag - dot_nt(lwin[at, s], lwin[at, s])
            diag[...] = new_diag

            def put_l(g, v):
                lt_c[i, 8 * g:8 * g + 8, :] = v

            def put_inv(g, v):
                linv_c[at, 8 * g:8 * g + 8, :] = v

            chol_inv(lambda g: diag[8 * g:8 * g + 8, :], put_l, put_inv)

            @pl.when(i >= 2)
            def _():
                drain_chain(i - 2)

            for r in range(row_procs):
                @pl.when(linv_goes(i, r))
                def _():
                    linv_copy(i, r).start()

                    @pl.when(i >= 1)
                    def _():
                        lnext_copy(i, r).start()
            ldiag_copy(i).start()
            return 0

        @pl.when(is_chain)
        def _():
            for m in range(slots):
                give(m).start()
            for i in range(RING):
                linv_c[i] = jnp.zeros((NB, NB), jnp.float32)
                for s in range(LAG):
                    lwin[i, s] = jnp.zeros((NB, NB), jnp.float32)
            for i in range(LAG):
                for s in range(LAG - i):
                    win[i, s] = jnp.zeros((NB, NB), jnp.float32)
            lax.fori_loop(0, steps, chain_step, 0)
            drain_chain(steps - 2)
            drain_chain(steps - 1)
            for m in range(slots):
                give(m).wait_send()
            for m in range(slots):
                dst = pan_out.at[m] if m < panel_dev else trl_out
                wait_recv(dst, outc_sem.at[m])

        num_virtual = jnp.where(is_sib, 2, 1)
        col_half = pc // row_procs
        z_me, y_me = pc // 2, lax.rem(pc, 2)
        is_col_src = pr == lax.rem(pc, row_procs)

        def row_of(v):
            return jnp.where(v == 0, pr, CHAIN_ROW)

        def first_block(k, r):
            return (k - r + row_procs) // row_procs

        def row_children(k):
            owner = lax.rem(k, col_procs)
            z_own, y_own = owner // 2, lax.rem(owner, 2)

            def parents(peer):
                z, y = peer // 2, lax.rem(peer, 2)
                along = jnp.where(z < z_own, z + 1, z - 1) * 2 + y
                across = z * 2 + 1 - y
                in_line = y == y_own
                at_own = z == z_own
                even = jnp.where(at_own, owner, jnp.where(in_line, along, across))
                odd = jnp.where(at_own, owner, jnp.where(in_line, across, along))
                return even, odd

            found = []
            for peer, valid in ((z_me * 2 + 1 - y_me, True), (pc + 2, z_me < col_procs // 2 - 1), (pc - 2, z_me > 0)):
                ok = jnp.logical_and(valid, peer != owner)
                even, odd = parents(jnp.maximum(peer, 0))
                found.append((jnp.logical_and(ok, even == pc), jnp.logical_and(ok, odd == pc), peer))
            return found

        def row_copy(k, v, l, c, peer):
            r = row_of(v)
            moved = jnp.logical_and(peer == CHAIN_COL, r == CHAIN_ROW)
            v_dst = jnp.where(moved, 1, 0)
            r_dst = jnp.where(moved, sib_row, r)
            return remote(rowp.at[v, k, rows(l)], rowp.at[v_dst, k, rows(l)], row_snd.at[lax.rem(k, 3), v, l, c],
                          row_sem.at[v_dst, k, l], (peer, r_dst))

        def col_copy(k, v, l, m, d):
            return remote(rowp.at[v, k, rows(l)], colp.at[k, rows(m)], col_snd.at[lax.rem(k, 3), m, d - 1],
                          col_sem.at[k, m], (pc, lax.rem(pr + d, row_procs)))

        def col_goes(d):
            return jnp.logical_not(jnp.logical_and(at_chain_col, lax.rem(pr + d, row_procs) == CHAIN_ROW))

        def needs_col(k, col_block):
            return jnp.logical_and(col_block > k, jnp.logical_or(col_block != k + 1, col_block >= steps))

        def is_col_block(k, v, l):
            here = jnp.logical_and(row_of(v) == lax.rem(pc, row_procs), lax.rem(l, 2) == col_half)
            return jnp.logical_and(here, needs_col(k, pc + (l // 2) * col_procs))

        def each_block(k, act):
            def virtual(v, _):
                def block(l, _):
                    act(v, l)
                    return 0
                return lax.fori_loop(first_block(k, row_of(v)), row_blocks, block, 0)
            lax.fori_loop(0, num_virtual, virtual, 0)

        def each_send(k, v, l, act, children):
            odd_row = lax.rem(row_of(v), 2) == 1
            for c, (even, odd, peer) in enumerate(children):
                @pl.when(jnp.where(odd_row, odd, even))
                def _():
                    act(row_copy(k, v, l, c, peer))

            @pl.when(is_col_block(k, v, l))
            def _():
                for d in range(1, row_procs):
                    @pl.when(col_goes(d))
                    def _():
                        act(col_copy(k, v, l, l // 2, d))

        def drain_sends(k):
            children = row_children(k)
            each_block(k, lambda v, l: each_send(k, v, l, lambda c: c.wait_send(), children))

        def stage_copy(v, i, s):
            return remote(stage.at[v, i // row_procs], win.at[i, s], stage_snd.at[v, i // row_procs], win_sem.at[i, s], chain_id)

        def entering(k, v):
            i = k + LAG + 1
            s = lax.rem(pc - (k + 1) + 4 * col_procs, col_procs)
            here = jnp.logical_and(jnp.logical_and(i < steps, s <= LAG), row_of(v) == lax.rem(i, row_procs))
            return here, i, s, (k + 1 + s) // col_procs

        def init_copy(i):
            return remote(pan_in.at[0, pl.ds((i // row_procs) * NB, NB)], win.at[i, jnp.clip(pc - i + LAG, 0, LAG)], init_snd.at[i],
                          win_sem.at[i, jnp.clip(pc - i + LAG, 0, LAG)], chain_id)

        def init_goes(i):
            return jnp.logical_and(pr == i % row_procs, pc <= i)

        def out_local(m):
            dst = pan_out.at[m] if m < panel_dev else trl_out
            return pltpu.make_async_copy(tile.at[0, m], dst, out_sem.at[m])

        def out_remote(m):
            dst = pan_out.at[m] if m < panel_dev else trl_out
            return remote(tile.at[1, m], dst, out_sem.at[slots + m], outc_sem.at[m], chain_id)

        def start_out(m):
            out_local(m).start()

            @pl.when(is_sib)
            def _():
                out_remote(m).start()

        has_src = jnp.logical_or(is_col_src, jnp.logical_and(is_sib, CHAIN_ROW == lax.rem(pc, row_procs)))

        def wait_col(k, m):
            wait_recv(colp.at[k, rows(m)], col_sem.at[k, m])

        def send_block(k, v, l, children):
            each_send(k, v, l, lambda c: c.start(), children)

            @pl.when(is_col_block(k, v, l))
            def _():
                colp[k, rows(l // 2), :] = rowp[v, k, rows(l), :]

        def enter(k, v):
            here, i, s, m = entering(k, v)

            @pl.when(jnp.logical_and(here, s > 1))
            def _():
                l = i // row_procs
                new = tile[v, m, rows(l), :] - dot_nt(rowp[v, k, rows(l), :], colp[k, rows(m), :])
                tile[v, m, rows(l), :] = new
                stage[v, l] = new
                stage_copy(v, i, s).start()

        def solve_next(k, v, l, first, children):
            m = (k + 1) // col_procs
            i = row_procs * l + row_of(v)
            new = tile[v, m, rows(l), :]
            if not first:
                prev = jnp.maximum(k - 1, 0)
                @pl.when(jnp.logical_and(k >= 1, jnp.logical_and(i == k + LAG, i < steps)))
                def _():
                    stage[v, l] = tile[v, m, rows(l), :] - dot_nt(rowp[v, prev, rows(l), :], colp[prev, rows(m), :])
                    stage_copy(v, i, 1).start()

                left = jnp.concatenate([jnp.where(k == 0, 0.0, rowp[v, prev, rows(l), :]), rowp[v, k, rows(l), :]], axis=1)
                right = jnp.concatenate([jnp.where(k == 0, 0.0, colp[prev, rows(m), :]), lnext_in[m]], axis=1)
                new = new - dot_nt(left, right)

                @pl.when(jnp.logical_and(i == k + LAG + 1, i < steps))
                def _():
                    stage[v, l] = new
                    stage_copy(v, i, 0).start()
            x = dot_nt(new, linv_in[m])
            rowp[v, k + 1, rows(l), :] = x
            tile[v, m, rows(l), :] = x
            send_block(k + 1, v, l, children)

        def update_row(q, v, l):
            r = row_of(v)
            i_row = row_procs * l + r
            upd = dot_nt(rowp[v, q, rows(l), :], colp[q])
            entered = jnp.logical_and(i_row == q + LAG + 1, i_row < steps)
            for m in range(slots):
                col_block = pc + m * col_procs
                take = jnp.logical_and(col_block > q, jnp.logical_or(col_block > q + 2, col_block >= steps))
                take = jnp.logical_and(take, jnp.logical_not(jnp.logical_and(entered, col_block <= i_row)))
                if m < panel_dev:
                    take = jnp.logical_and(take, i_row >= col_block)

                @pl.when(take)
                def _():
                    tile[v, m, rows(l), :] = tile[v, m, rows(l), :] - upd[:, m * NB:(m + 1) * NB]

        def owner_step(k, _):
            own = jnp.logical_and(pc == lax.rem(k, col_procs), k < steps)
            own_next = jnp.logical_and(pc == lax.rem(k + 1, col_procs), k + 1 < steps)
            m_own = k // col_procs
            m_next = (k + 1) // col_procs
            children = row_children(k)
            children_next = row_children(k + 1)

            @pl.when(k >= 2)
            def _():
                drain_sends(k - 2)

            @pl.when(own_next)
            def _():
                wait_recv(linv_in.at[m_next], linv_sem.at[m_next])
                wait_recv(lnext_in.at[m_next], lnext_sem.at[m_next])

                @pl.when(jnp.logical_and(jnp.logical_not(has_src), k >= 1))
                def _():
                    wait_col(k - 1, m_next)

            def row(t, _):
                @pl.when(jnp.logical_and(t == BEHIND, k >= 1))
                def _():
                    for m in range(slots):
                        col_block = pc + m * col_procs
                        due = jnp.logical_and(needs_col(k - 1, col_block), jnp.logical_not(jnp.logical_and(own_next, m == m_next)))

                        @pl.when(jnp.logical_and(due, jnp.logical_not(has_src)))
                        def _():
                            wait_col(k - 1, m)

                    def window(v, _):
                        enter(k - 1, v)
                        return 0

                    lax.fori_loop(0, num_virtual, window, 0)

                def virtual(v, _):
                    r = row_of(v)
                    l = k // row_procs + t

                    @pl.when(jnp.logical_and(jnp.logical_and(l < row_blocks, l >= first_block(k, r)), k < steps))
                    def _():
                        @pl.when(jnp.logical_not(own))
                        def _():
                            wait_recv(rowp.at[v, k, rows(l)], row_sem.at[v, k, l])
                            send_block(k, v, l, children)

                        @pl.when(jnp.logical_and(own_next, row_procs * l + r > k + 1))
                        def _():
                            solve_next(k, v, l, False, children_next)

                    l_upd = l - BEHIND

                    @pl.when(jnp.logical_and(jnp.logical_and(t >= BEHIND, k >= 1), l_upd >= first_block(k - 1, r)))
                    def _():
                        update_row(k - 1, v, l_upd)
                    return 0

                return lax.fori_loop(0, num_virtual, virtual, 0)

            lax.fori_loop(0, row_blocks + BEHIND - k // row_procs, row, 0)

            @pl.when(own)
            def _():
                def finish(v, _):
                    r = row_of(v)

                    @pl.when(r == lax.rem(k, row_procs))
                    def _():
                        wait_recv(ldiag_in.at[m_own], ldiag_sem.at[m_own])
                        tile[v, m_own, rows(k // row_procs), :] = jnp.transpose(ldiag_in[m_own])

                    def clear(l, _):
                        tile[v, m_own, rows(l), :] = jnp.zeros((NB, NB), jnp.float32)
                        return 0

                    lax.fori_loop(0, (k - r + row_procs - 1) // row_procs, clear, 0)
                    return 0

                lax.fori_loop(0, num_virtual, finish, 0)
                for m in range(panel_dev):
                    @pl.when(m_own == m)
                    def _():
                        start_out(m)
            return 0

        def first_column():
            wait_recv(linv_in.at[0], linv_sem.at[0])
            children = row_children(0)

            def virtual(v, _):
                def block(l, _):
                    solve_next(-1, v, l, True, children)
                    return 0
                return lax.fori_loop(first_block(0, row_of(v)), row_blocks, block, 0)
            lax.fori_loop(0, num_virtual, virtual, 0)

        @pl.when(jnp.logical_not(is_chain))
        def _():
            for i in range(LAG + 1):
                @pl.when(init_goes(i))
                def _():
                    init_copy(i).start()
            for m in range(slots):
                load(m).wait()

            @pl.when(is_sib)
            def _():
                for m in range(slots):
                    wait_recv(tile.at[1, m], give_sem.at[m])

            @pl.when(pc == 0)
            def _():
                first_column()

            lax.fori_loop(0, steps + 1, owner_step, 0)
            start_out(panel_dev)
            drain_sends(steps - 1)
            for i in range(LAG + 1):
                @pl.when(init_goes(i))
                def _():
                    init_copy(i).wait_send()

            def drain_stage(k, _):
                def virtual(v, _):
                    here, i, s, m = entering(k, v)

                    @pl.when(here)
                    def _():
                        stage_copy(v, i, s).wait_send()
                    return 0
                return lax.fori_loop(0, num_virtual, virtual, 0)

            lax.fori_loop(0, steps, drain_stage, 0)
            for m in range(slots):
                out_local(m).wait()

                @pl.when(is_sib)
                def _():
                    out_remote(m).wait_send()

    return kernel


def solution(mesh):
    row_procs = mesh.shape["pr"]
    col_procs = mesh.shape["pc"]

    def local_part(panel_tile, trail_tile):
        local_rows, panel_dev, _ = panel_tile.shape
        steps = panel_dev * col_procs
        row_blocks = local_rows // NB
        slots = panel_dev + 1
        f32 = jnp.float32
        dma = pltpu.SemaphoreType.DMA
        scratch = [
            pltpu.VMEM((2, slots, local_rows, NB), f32),
            pltpu.VMEM((2, steps, local_rows, NB), f32),
            pltpu.VMEM((steps, slots * NB, NB), f32),
            pltpu.VMEM((panel_dev, NB, NB), f32),
            pltpu.VMEM((panel_dev, NB, NB), f32),
            pltpu.VMEM((panel_dev, NB, NB), f32),
            pltpu.VMEM((2, steps // row_procs, NB, NB), f32),
            pltpu.VMEM((steps, LAG + 1, NB, NB), f32),
            pltpu.VMEM((RING, LAG, NB, NB), f32),
            pltpu.VMEM((RING, NB, NB), f32),
            pltpu.VMEM((steps, NB, NB), f32),
            pltpu.VMEM((NB, NB), f32),
            dma((slots,)),
            dma((2, steps, row_blocks)),
            dma((steps, slots)),
            dma((panel_dev,)),
            dma((panel_dev,)),
            dma((panel_dev,)),
            dma((steps, LAG + 1)),
            dma((slots,)),
            dma((2 * slots,)),
            dma((3, 2, row_blocks, 3)),
            dma((3, slots, row_procs - 1)),
            dma((2, steps // row_procs)),
            dma((LAG + 1,)),
            dma((2, row_procs)),
            dma((2, row_procs)),
            dma((2,)),
            dma((slots,)),
            dma((slots,)),
        ]
        hbm = pl.BlockSpec(memory_space=pl.ANY)
        by_slot = jnp.transpose(panel_tile, (1, 0, 2))
        panel_new, trail_new = pl.pallas_call(
            make_kernel(row_procs, col_procs, local_rows, panel_dev),
            out_shape=[jax.ShapeDtypeStruct(by_slot.shape, f32), jax.ShapeDtypeStruct(trail_tile.shape, f32)],
            in_specs=[hbm, hbm],
            out_specs=[hbm, hbm],
            scratch_shapes=scratch,
            compiler_params=pltpu.CompilerParams(collective_id=0, has_side_effects=True, vmem_limit_bytes=67043328),
        )(by_slot, trail_tile)
        return jnp.transpose(panel_new, (1, 0, 2)), trail_new

    spec_panel = P("pr", "pc", None)
    spec_trail = P("pr", "pc")
    return jax.shard_map(local_part, mesh=mesh, in_specs=(spec_panel, spec_trail), out_specs=(spec_panel, spec_trail), check_vma=False)
```

```python
import jax
import jax.numpy as jnp
from jax import lax
from jax.experimental import pallas as pl
from jax.experimental.pallas import tpu as pltpu
from jax.sharding import PartitionSpec as P

MESH = pl.DeviceIdType.MESH
PREC_HIGH = lax.Precision.HIGHEST
NB = 128
LAG = 4
CHAIN_COL = 4
CHAIN_ROW = 1
RING = 8
BEHIND = 2
PIECES = 1


def _sub_bcast(v, s):
    return jnp.broadcast_to(v[s:s + 1, :], (8, NB))


def _lane_bcast(v, c):
    return jnp.broadcast_to(v[:, c:c + 1], (8, NB))


def chol_inv(load, store_l, store_inv, q=2):
    ng = NB // 8
    step = 8 * q
    x = [load(g) for g in range(ng)]
    row_id = lax.broadcasted_iota(jnp.int32, (8, NB), 0)
    col_id = lax.broadcasted_iota(jnp.int32, (8, NB), 1)
    y = [jnp.where(col_id == row_id + 8 * g, 1.0, 0.0) for g in range(ng)]
    for b in range(NB // step):
        g0 = b * q
        c0 = b * step
        last = b == NB // step - 1
        e = [[_lane_bcast(x[g0 + s], c0 + t) if 8 * (s + 1) > t else None for s in range(q)] for t in range(step)]
        p = None
        if not last:
            p = [[_lane_bcast(x[g0 + q + s], c0 + t) for s in range(q)] for t in range(step)]
        rr = [None] * q
        ss = [None] * q
        rows = []
        for t in range(step):
            gt, st = t // 8, t % 8
            d = _sub_bcast(e[t][gt], st)
            r = lax.rsqrt(d)
            col = [e[t][s] * r if s >= gt else None for s in range(q)]
            rt = _sub_bcast(x[g0 + gt], st) * r
            sr = _sub_bcast(y[g0 + gt], st) * r
            rows.append((rt, sr))
            if st == 0:
                rr[gt], ss[gt] = rt, sr
            else:
                rr[gt] = jnp.where(row_id == st, rt, rr[gt])
                ss[gt] = jnp.where(row_id == st, sr, ss[gt])
            for s in range(gt, q):
                x[g0 + s] = x[g0 + s] - col[s] * rt
                y[g0 + s] = y[g0 + s] - col[s] * sr
            pc = None
            if not last:
                pc = [p[t][s] * r for s in range(q)]
                for s in range(q):
                    x[g0 + q + s] = x[g0 + q + s] - pc[s] * rt
                    y[g0 + q + s] = y[g0 + q + s] - pc[s] * sr
            for u in range(t + 1, step):
                w = _sub_bcast(col[u // 8], u % 8)
                for s in range(u // 8, q):
                    e[u][s] = e[u][s] - col[s] * w
                if not last:
                    for s in range(q):
                        p[u][s] = p[u][s] - pc[s] * w
        for s in range(q):
            store_l(g0 + s, jnp.where(col_id >= row_id + 8 * (g0 + s), rr[s], 0.0))
            store_inv(g0 + s, jnp.where(col_id <= row_id + 8 * (g0 + s), ss[s], 0.0))
        if b < NB // step - 2:
            for s in range(q):
                rt_t = jnp.transpose(rr[s])
                for g in range(g0 + 2 * q, ng):
                    blk = rt_t[8 * g:8 * g + 8, :]
                    for st in range(8):
                        m = jnp.broadcast_to(blk[:, st:st + 1], (8, NB))
                        rt, sr = rows[8 * s + st]
                        x[g] = x[g] - m * rt
                        y[g] = y[g] - m * sr


def dot_nt(a, b):
    return lax.dot_general(a, b, (((1,), (1,)), ((), ())), precision=PREC_HIGH, preferred_element_type=jnp.float32)


def make_kernel(row_procs, col_procs, local_rows, panel_dev):
    steps = panel_dev * col_procs
    row_blocks = local_rows // NB
    slots = panel_dev + 1
    half = row_blocks // 2
    sib_row = CHAIN_ROW ^ 1

    def kernel(pan_in, trl_in, pan_out, trl_out, tile, rowp, colp, linv_in, lnext_in, ldiag_in, stage, win, lwin, linv_c, lt_c, diag,
               in_sem, row_sem, col_sem, linv_sem, lnext_sem, ldiag_sem, win_sem, outc_sem, out_sem,
               row_snd, col_snd, stage_snd, init_snd, linv_snd, lnext_snd, ldiag_snd, give_snd, give_sem):
        pc = lax.axis_index("pc")
        pr = lax.axis_index("pr")
        at_chain_col = pc == CHAIN_COL
        is_chain = jnp.logical_and(at_chain_col, pr == CHAIN_ROW)
        is_sib = jnp.logical_and(at_chain_col, pr == sib_row)
        chain_id = (CHAIN_COL, CHAIN_ROW)
        sib_id = (CHAIN_COL, sib_row)
        some_other = (pc, pr ^ 1)

        def rows(l):
            return pl.ds(pl.multiple_of(l * NB, NB), NB)

        def piece(l, h):
            return pl.ds(pl.multiple_of(l * NB + h * (NB // PIECES), NB // PIECES), NB // PIECES)

        def remote(src, dst, snd, rcv, dev):
            return pltpu.make_async_remote_copy(src_ref=src, dst_ref=dst, send_sem=snd, recv_sem=rcv, device_id=dev, device_id_type=MESH)

        def wait_recv(ref, rcv):
            remote(ref, ref, give_snd.at[0], rcv, some_other).wait_recv()

        barrier = pltpu.get_barrier_semaphore()
        total = row_procs * col_procs
        me = pc * row_procs + pr

        def greet(d, _):
            other = lax.rem(me + d, total)
            pl.semaphore_signal(barrier, inc=1, device_id=(other // row_procs, lax.rem(other, row_procs)), device_id_type=MESH)
            return 0

        def load(m):
            src = pan_in.at[m] if m < panel_dev else trl_in
            return pltpu.make_async_copy(src, tile.at[0, m], in_sem.at[m])

        @pl.when(jnp.logical_not(is_chain))
        def _():
            for m in range(slots):
                load(m).start()

        lax.fori_loop(1, total, greet, 0)
        pl.semaphore_wait(barrier, total - 1)

        def give(m):
            src = pan_in.at[m] if m < panel_dev else trl_in
            return remote(src, tile.at[1, m], give_snd.at[m], give_sem.at[m], sib_id)

        def linv_copy(i, r):
            return remote(linv_c.at[lax.rem(i, RING)], linv_in.at[i // col_procs], linv_snd.at[lax.rem(i, 2), r], linv_sem.at[i // col_procs],
                          (lax.rem(i, col_procs), r))

        def linv_goes(i, r):
            return jnp.logical_or(lax.rem(i, col_procs) != CHAIN_COL, r != CHAIN_ROW)

        def lnext_copy(i, r):
            return remote(lwin.at[lax.rem(i, RING), LAG - 1], lnext_in.at[i // col_procs], lnext_snd.at[lax.rem(i, 2), r],
                          lnext_sem.at[i // col_procs], (lax.rem(i, col_procs), r))

        def ldiag_copy(i):
            return remote(lt_c.at[i], ldiag_in.at[i // col_procs], ldiag_snd.at[lax.rem(i, 2)], ldiag_sem.at[i // col_procs],
                          (lax.rem(i, col_procs), lax.rem(i, row_procs)))

        def drain_chain(i):
            for r in range(row_procs):
                @pl.when(linv_goes(i, r))
                def _():
                    linv_copy(i, r).wait_send()

                    @pl.when(i >= 1)
                    def _():
                        lnext_copy(i, r).wait_send()
            ldiag_copy(i).wait_send()

        def chain_step(i, _):
            for s in range(LAG + 1):
                @pl.when(i - LAG + s >= 0)
                def _():
                    wait_recv(win.at[i, s], win_sem.at[i, s])
            at = lax.rem(i, RING)
            old = [lax.rem(i + RING - LAG + s, RING) for s in range(LAG)]
            for s in range(LAG):
                acc = win[i, s]
                for q in range(s):
                    acc = acc - dot_nt(lwin[at, q], lwin[old[s], LAG - s + q])
                lwin[at, s] = dot_nt(acc, linv_c[old[s]])
            new_diag = win[i, LAG]
            for s in range(LAG):
                new_diag = new_diag - dot_nt(lwin[at, s], lwin[at, s])
            diag[...] = new_diag

            def put_l(g, v):
                lt_c[i, 8 * g:8 * g + 8, :] = v

            def put_inv(g, v):
                linv_c[at, 8 * g:8 * g + 8, :] = v

            chol_inv(lambda g: diag[8 * g:8 * g + 8, :], put_l, put_inv)

            @pl.when(i >= 2)
            def _():
                drain_chain(i - 2)

            for r in range(row_procs):
                @pl.when(linv_goes(i, r))
                def _():
                    linv_copy(i, r).start()

                    @pl.when(i >= 1)
                    def _():
                        lnext_copy(i, r).start()
            ldiag_copy(i).start()
            return 0

        @pl.when(is_chain)
        def _():
            for m in range(slots):
                give(m).start()
            for i in range(RING):
                linv_c[i] = jnp.zeros((NB, NB), jnp.float32)
                for s in range(LAG):
                    lwin[i, s] = jnp.zeros((NB, NB), jnp.float32)
            for i in range(LAG):
                for s in range(LAG - i):
                    win[i, s] = jnp.zeros((NB, NB), jnp.float32)
            lax.fori_loop(0, steps, chain_step, 0)
            drain_chain(steps - 2)
            drain_chain(steps - 1)
            for m in range(slots):
                give(m).wait_send()
            for m in range(slots):
                dst = pan_out.at[m] if m < panel_dev else trl_out
                wait_recv(dst, outc_sem.at[m])

        num_virtual = jnp.where(is_sib, 2, 1)
        col_half = pc // row_procs
        z_me, y_me = pc // 2, lax.rem(pc, 2)
        is_col_src = pr == lax.rem(pc, row_procs)

        def row_of(v):
            return jnp.where(v == 0, pr, CHAIN_ROW)

        def first_block(k, r):
            return (k - r + row_procs) // row_procs

        def row_children(k):
            owner = lax.rem(k, col_procs)
            z_own = owner // 2

            def parent(peer):
                z, y = peer // 2, lax.rem(peer, 2)
                return jnp.where(z == z_own, owner, jnp.where(z < z_own, z + 1, z - 1) * 2 + y)

            found = []
            for peer, valid in ((z_me * 2 + 1 - y_me, True), (pc + 2, z_me < col_procs // 2 - 1), (pc - 2, z_me > 0)):
                ok = jnp.logical_and(valid, peer != owner)
                found.append((jnp.logical_and(ok, parent(jnp.maximum(peer, 0)) == pc), peer))
            return found

        def row_copy(k, v, l, h, c, peer):
            r = row_of(v)
            moved = jnp.logical_and(peer == CHAIN_COL, r == CHAIN_ROW)
            v_dst = jnp.where(moved, 1, 0)
            r_dst = jnp.where(moved, sib_row, r)
            return remote(rowp.at[v, k, piece(l, h)], rowp.at[v_dst, k, piece(l, h)], row_snd.at[lax.rem(k, 3), v, l * PIECES + h, c],
                          row_sem.at[v_dst, k, l * PIECES + h], (peer, r_dst))

        def col_copy(k, v, l, m, d):
            return remote(rowp.at[v, k, rows(l)], colp.at[k, rows(m)], col_snd.at[lax.rem(k, 3), m, d - 1],
                          col_sem.at[k, m], (pc, lax.rem(pr + d, row_procs)))

        def col_goes(d):
            return jnp.logical_not(jnp.logical_and(at_chain_col, lax.rem(pr + d, row_procs) == CHAIN_ROW))

        def needs_col(k, col_block):
            return jnp.logical_and(col_block > k, jnp.logical_or(col_block != k + 1, col_block >= steps))

        def is_col_block(k, v, l):
            here = jnp.logical_and(row_of(v) == lax.rem(pc, row_procs), lax.rem(l, 2) == col_half)
            return jnp.logical_and(here, needs_col(k, pc + (l // 2) * col_procs))

        def each_block(k, act):
            def virtual(v, _):
                def block(l, _):
                    act(v, l)
                    return 0
                return lax.fori_loop(first_block(k, row_of(v)), row_blocks, block, 0)
            lax.fori_loop(0, num_virtual, virtual, 0)

        def each_send(k, v, l, act, children):
            for h in range(PIECES):
                send_piece(k, v, l, h, act, children)
            send_col(k, v, l, act)

        def send_piece(k, v, l, h, act, children):
            for c, (goes, peer) in enumerate(children):
                @pl.when(goes)
                def _():
                    act(row_copy(k, v, l, h, c, peer))

        def send_col(k, v, l, act):
            @pl.when(is_col_block(k, v, l))
            def _():
                for d in range(1, row_procs):
                    @pl.when(col_goes(d))
                    def _():
                        act(col_copy(k, v, l, l // 2, d))

        def drain_sends(k):
            children = row_children(k)
            each_block(k, lambda v, l: each_send(k, v, l, lambda c: c.wait_send(), children))

        def stage_copy(v, i, s):
            return remote(stage.at[v, i // row_procs], win.at[i, s], stage_snd.at[v, i // row_procs], win_sem.at[i, s], chain_id)

        def entering(k, v):
            i = k + LAG + 1
            s = lax.rem(pc - (k + 1) + 4 * col_procs, col_procs)
            here = jnp.logical_and(jnp.logical_and(i < steps, s <= LAG), row_of(v) == lax.rem(i, row_procs))
            return here, i, s, (k + 1 + s) // col_procs

        def init_copy(i):
            return remote(pan_in.at[0, pl.ds((i // row_procs) * NB, NB)], win.at[i, jnp.clip(pc - i + LAG, 0, LAG)], init_snd.at[i],
                          win_sem.at[i, jnp.clip(pc - i + LAG, 0, LAG)], chain_id)

        def init_goes(i):
            return jnp.logical_and(pr == i % row_procs, pc <= i)

        def out_local(m):
            dst = pan_out.at[m] if m < panel_dev else trl_out
            return pltpu.make_async_copy(tile.at[0, m], dst, out_sem.at[m])

        def out_remote(m):
            dst = pan_out.at[m] if m < panel_dev else trl_out
            return remote(tile.at[1, m], dst, out_sem.at[slots + m], outc_sem.at[m], chain_id)

        def start_out(m):
            out_local(m).start()

            @pl.when(is_sib)
            def _():
                out_remote(m).start()

        has_src = jnp.logical_or(is_col_src, jnp.logical_and(is_sib, CHAIN_ROW == lax.rem(pc, row_procs)))

        def wait_col(k, m):
            wait_recv(colp.at[k, rows(m)], col_sem.at[k, m])

        def share_col(k, v, l):
            send_col(k, v, l, lambda c: c.start())

            @pl.when(is_col_block(k, v, l))
            def _():
                colp[k, rows(l // 2), :] = rowp[v, k, rows(l), :]

        def enter(k, v):
            here, i, s, m = entering(k, v)

            @pl.when(jnp.logical_and(here, s > 1))
            def _():
                l = i // row_procs
                new = tile[v, m, rows(l), :] - dot_nt(rowp[v, k, rows(l), :], colp[k, rows(m), :])
                tile[v, m, rows(l), :] = new
                stage[v, l] = new
                stage_copy(v, i, s).start()

        def solve_next(k, v, l, first, children):
            m = (k + 1) // col_procs
            i = row_procs * l + row_of(v)
            new = tile[v, m, rows(l), :]
            if not first:
                prev = jnp.maximum(k - 1, 0)
                @pl.when(jnp.logical_and(k >= 1, jnp.logical_and(i == k + LAG, i < steps)))
                def _():
                    stage[v, l] = tile[v, m, rows(l), :] - dot_nt(rowp[v, prev, rows(l), :], colp[prev, rows(m), :])
                    stage_copy(v, i, 1).start()

                left = jnp.concatenate([jnp.where(k == 0, 0.0, rowp[v, prev, rows(l), :]), rowp[v, k, rows(l), :]], axis=1)
                right = jnp.concatenate([jnp.where(k == 0, 0.0, colp[prev, rows(m), :]), lnext_in[m]], axis=1)
                new = new - dot_nt(left, right)

                @pl.when(jnp.logical_and(i == k + LAG + 1, i < steps))
                def _():
                    stage[v, l] = new
                    stage_copy(v, i, 0).start()
            x = dot_nt(new, linv_in[m])
            rowp[v, k + 1, rows(l), :] = x
            tile[v, m, rows(l), :] = x
            for h in range(PIECES):
                send_piece(k + 1, v, l, h, lambda c: c.start(), children)
            share_col(k + 1, v, l)

        def update_row(q, v, l):
            r = row_of(v)
            i_row = row_procs * l + r
            upd = dot_nt(rowp[v, q, rows(l), :], colp[q])
            entered = jnp.logical_and(i_row == q + LAG + 1, i_row < steps)
            for m in range(slots):
                col_block = pc + m * col_procs
                take = jnp.logical_and(col_block > q, jnp.logical_or(col_block > q + 2, col_block >= steps))
                take = jnp.logical_and(take, jnp.logical_not(jnp.logical_and(entered, col_block <= i_row)))
                if m < panel_dev:
                    take = jnp.logical_and(take, i_row >= col_block)

                @pl.when(take)
                def _():
                    tile[v, m, rows(l), :] = tile[v, m, rows(l), :] - upd[:, m * NB:(m + 1) * NB]

        def owner_step(k, _):
            own = jnp.logical_and(pc == lax.rem(k, col_procs), k < steps)
            own_next = jnp.logical_and(pc == lax.rem(k + 1, col_procs), k + 1 < steps)
            m_own = k // col_procs
            m_next = (k + 1) // col_procs
            children = row_children(k)
            children_next = row_children(k + 1)

            @pl.when(k >= 2)
            def _():
                drain_sends(k - 2)

            @pl.when(own_next)
            def _():
                wait_recv(linv_in.at[m_next], linv_sem.at[m_next])
                wait_recv(lnext_in.at[m_next], lnext_sem.at[m_next])

                @pl.when(jnp.logical_and(jnp.logical_not(has_src), k >= 1))
                def _():
                    wait_col(k - 1, m_next)

            def row(t, _):
                @pl.when(jnp.logical_and(t == BEHIND, k >= 1))
                def _():
                    for m in range(slots):
                        col_block = pc + m * col_procs
                        due = jnp.logical_and(needs_col(k - 1, col_block), jnp.logical_not(jnp.logical_and(own_next, m == m_next)))

                        @pl.when(jnp.logical_and(due, jnp.logical_not(has_src)))
                        def _():
                            wait_col(k - 1, m)

                    def window(v, _):
                        enter(k - 1, v)
                        return 0

                    lax.fori_loop(0, num_virtual, window, 0)

                def virtual(v, _):
                    r = row_of(v)
                    l = k // row_procs + t

                    @pl.when(jnp.logical_and(jnp.logical_and(l < row_blocks, l >= first_block(k, r)), k < steps))
                    def _():
                        @pl.when(jnp.logical_not(own))
                        def _():
                            for h in range(PIECES):
                                wait_recv(rowp.at[v, k, piece(l, h)], row_sem.at[v, k, l * PIECES + h])
                                send_piece(k, v, l, h, lambda c: c.start(), children)
                            share_col(k, v, l)

                        @pl.when(jnp.logical_and(own_next, row_procs * l + r > k + 1))
                        def _():
                            solve_next(k, v, l, False, children_next)

                    l_upd = l - BEHIND

                    @pl.when(jnp.logical_and(jnp.logical_and(t >= BEHIND, k >= 1), l_upd >= first_block(k - 1, r)))
                    def _():
                        update_row(k - 1, v, l_upd)
                    return 0

                return lax.fori_loop(0, num_virtual, virtual, 0)

            lax.fori_loop(0, row_blocks + BEHIND - k // row_procs, row, 0)

            @pl.when(own)
            def _():
                def finish(v, _):
                    r = row_of(v)

                    @pl.when(r == lax.rem(k, row_procs))
                    def _():
                        wait_recv(ldiag_in.at[m_own], ldiag_sem.at[m_own])
                        tile[v, m_own, rows(k // row_procs), :] = jnp.transpose(ldiag_in[m_own])

                    def clear(l, _):
                        tile[v, m_own, rows(l), :] = jnp.zeros((NB, NB), jnp.float32)
                        return 0

                    lax.fori_loop(0, (k - r + row_procs - 1) // row_procs, clear, 0)
                    return 0

                lax.fori_loop(0, num_virtual, finish, 0)
                for m in range(panel_dev):
                    @pl.when(m_own == m)
                    def _():
                        start_out(m)
            return 0

        def first_column():
            wait_recv(linv_in.at[0], linv_sem.at[0])
            children = row_children(0)

            def virtual(v, _):
                def block(l, _):
                    solve_next(-1, v, l, True, children)
                    return 0
                return lax.fori_loop(first_block(0, row_of(v)), row_blocks, block, 0)
            lax.fori_loop(0, num_virtual, virtual, 0)

        @pl.when(jnp.logical_not(is_chain))
        def _():
            for i in range(LAG + 1):
                @pl.when(init_goes(i))
                def _():
                    init_copy(i).start()
            for m in range(slots):
                load(m).wait()

            @pl.when(is_sib)
            def _():
                for m in range(slots):
                    wait_recv(tile.at[1, m], give_sem.at[m])

            @pl.when(pc == 0)
            def _():
                first_column()

            lax.fori_loop(0, steps + 1, owner_step, 0)
            start_out(panel_dev)
            drain_sends(steps - 1)
            for i in range(LAG + 1):
                @pl.when(init_goes(i))
                def _():
                    init_copy(i).wait_send()

            def drain_stage(k, _):
                def virtual(v, _):
                    here, i, s, m = entering(k, v)

                    @pl.when(here)
                    def _():
                        stage_copy(v, i, s).wait_send()
                    return 0
                return lax.fori_loop(0, num_virtual, virtual, 0)

            lax.fori_loop(0, steps, drain_stage, 0)
            for m in range(slots):
                out_local(m).wait()

                @pl.when(is_sib)
                def _():
                    out_remote(m).wait_send()

    return kernel


def solution(mesh):
    row_procs = mesh.shape["pr"]
    col_procs = mesh.shape["pc"]

    def local_part(panel_tile, trail_tile):
        local_rows, panel_dev, _ = panel_tile.shape
        steps = panel_dev * col_procs
        row_blocks = local_rows // NB
        slots = panel_dev + 1
        f32 = jnp.float32
        dma = pltpu.SemaphoreType.DMA
        scratch = [
            pltpu.VMEM((2, slots, local_rows, NB), f32),
            pltpu.VMEM((2, steps, local_rows, NB), f32),
            pltpu.VMEM((steps, slots * NB, NB), f32),
            pltpu.VMEM((panel_dev, NB, NB), f32),
            pltpu.VMEM((panel_dev, NB, NB), f32),
            pltpu.VMEM((panel_dev, NB, NB), f32),
            pltpu.VMEM((2, steps // row_procs, NB, NB), f32),
            pltpu.VMEM((steps, LAG + 1, NB, NB), f32),
            pltpu.VMEM((RING, LAG, NB, NB), f32),
            pltpu.VMEM((RING, NB, NB), f32),
            pltpu.VMEM((steps, NB, NB), f32),
            pltpu.VMEM((NB, NB), f32),
            dma((slots,)),
            dma((2, steps, row_blocks * PIECES)),
            dma((steps, slots)),
            dma((panel_dev,)),
            dma((panel_dev,)),
            dma((panel_dev,)),
            dma((steps, LAG + 1)),
            dma((slots,)),
            dma((2 * slots,)),
            dma((3, 2, row_blocks * PIECES, 3)),
            dma((3, slots, row_procs - 1)),
            dma((2, steps // row_procs)),
            dma((LAG + 1,)),
            dma((2, row_procs)),
            dma((2, row_procs)),
            dma((2,)),
            dma((slots,)),
            dma((slots,)),
        ]
        hbm = pl.BlockSpec(memory_space=pl.ANY)
        by_slot = jnp.transpose(panel_tile, (1, 0, 2))
        panel_new, trail_new = pl.pallas_call(
            make_kernel(row_procs, col_procs, local_rows, panel_dev),
            out_shape=[jax.ShapeDtypeStruct(by_slot.shape, f32), jax.ShapeDtypeStruct(trail_tile.shape, f32)],
            in_specs=[hbm, hbm],
            out_specs=[hbm, hbm],
            scratch_shapes=scratch,
            compiler_params=pltpu.CompilerParams(collective_id=0, has_side_effects=True, vmem_limit_bytes=67043328),
        )(by_slot, trail_tile)
        return jnp.transpose(panel_new, (1, 0, 2)), trail_new

    spec_panel = P("pr", "pc", None)
    spec_trail = P("pr", "pc")
    return jax.shard_map(local_part, mesh=mesh, in_specs=(spec_panel, spec_trail), out_specs=(spec_panel, spec_trail), check_vma=False)
```
